32 devices in a mesh: rep: 4 (over z), tp: 2 (over x), seq: 4 (over y, core).
Axes of the slice: x: 2, y: 2, z: 4, core: 2. Of those that a mesh axis runs over, the one named last changes fastest.
Arguments:
- prompt_x: bfloat16 [4, 4096, 8192], P('rep', 'seq'), may hold values from -6 to 6
- norm_gain: float32 [8192], replicated, may hold values from 0.1 to 1.9
- key_weight: bfloat16 [8192, 1024], P(None, 'tp'), may hold values from -0.0625 to 0.0625
- value_weight: bfloat16 [8192, 1024], P(None, 'tp'), may hold values from -0.0625 to 0.0625
- prompt_lengths: int32 [4], replicated, may hold values from 1024 to 4096
- page_table: int32 [4, 32], replicated, may hold values from 0 to 127, as said below
- request_slots: int32 [128], replicated, may hold values from 0 to 3
- queries: bfloat16 [4, 128, 8192], P(None, None, 'tp'), may hold values from -240 to 240
- new_kv: bfloat16 [2, 4, 128, 1024], P(None, None, ('rep', 'seq')), may hold values from -6 to 6
Outputs:
- attention: bfloat16 [4, 128, 8192], P(None, ('rep', 'seq'), 'tp')
- paged_cache: bfloat16 [128, 2, 128, 1024], P(('rep', 'seq'), None, None, 'tp')
The draws below stay inside these ranges and needn't reach their ends.
Inputs may be any that keep to these rules, and one draw needn't show every extreme that they name: `page_table`: every page 0 to 127 is named once; page // 8 is the decode shard (index of rep times 4 plus index of seq) that holds it; the blocks b * 8 to b * 8 + 7 of one prompt go to 8 different shards. `request_slots`: several requests may continue one prompt. `prompt_lengths`: tokens at or past a prompt's length are padding.
All inputs are finite; a program needn't handle non-finite values.
Results may differ from the reference program's by a relative error of at most 0.02.
The reference program's roundings to bfloat16 on the way count: a program that leaves them out, or rounds other values in their place, can miss the bound.
Values may be sent and summed in bfloat16 or wider, within the bound.
A program may use at most 192 MiB of HBM per device.

```python
import jax
import jax.numpy as jnp
from jax import lax

D = 8192
QH = 64
KVH = 8
HD = 128
BLK = 128
BPD = 8
STEPS = 4
PROMPTS = 4
SHARDS = 16
REPL = 1
KV_COLS = 1024
BLOCKS = 32
PLEN = 4096
PAGES = 128
REQS = 128


def draw_page_table(key, part):
    first_key, second_key, third_key = jax.random.split(jax.random.fold_in(key, 11), 3)
    order_dest = jax.random.permutation(first_key, SHARDS)
    order_src = jax.random.permutation(second_key, SHARDS)
    slot_order = jax.random.permutation(third_key, jnp.tile(jnp.arange(BPD, dtype=jnp.int32), (SHARDS, 1)), axis=1, independent=True)
    targets = order_dest[(order_src[:, None] + slot_order) % SHARDS]
    return (targets * BPD + slot_order).reshape(PROMPTS, BLOCKS).astype(jnp.int32)


def draw_queries(key, part):
    base_key = jax.random.fold_in(jax.random.fold_in(key, 23), 0)
    drawn = jax.random.truncated_normal(base_key, -6.0, 6.0, (STEPS, REQS, QH * HD), jnp.float32)
    return drawn.astype(jnp.bfloat16)


def touch_ends(entries, rng, low, high):
    longest = entries.shape.index(max(entries.shape))
    spots = []
    for shift in (0, 1):
        where = [jax.random.randint(jax.random.fold_in(rng, axis), (), 0, length) for axis, length in enumerate(entries.shape)]
        where[longest] = (where[longest] + shift) % entries.shape[longest]
        spots.append(tuple(where))
    return entries.at[spots[0]].set(low).at[spots[1]].set(high)


def levels(key, shape, pieces, low, top_value):
    def one(position, parts):
        draws = jax.random.uniform(jax.random.fold_in(jax.random.fold_in(key, 6), position), (parts,), jnp.float32, low / len(pieces), top_value / len(pieces))
        return jnp.repeat(jnp.exp(draws), shape[position] // parts).reshape((-1,) + (1,) * (len(shape) - position - 1))

    factor_of = one(*pieces[0])
    for cut in pieces[1:]:
        factor_of = factor_of * one(*cut)
    return factor_of


def noise(own_key, extent, deviation, most, cuts=(), held_as=jnp.bfloat16):
    values = deviation * jax.random.normal(own_key, extent, jnp.float32)
    if cuts:
        values = values * levels(own_key, extent, cuts, -0.22, 0.18)
    return jnp.clip(values, -most, most).astype(held_as)


def setup_inputs(seed: int = 0) -> dict:
    key_of = jax.random.split(jax.random.key(seed), 10)
    prompt_x = noise(key_of[0], (PROMPTS, PLEN, D), 1.0, 6.0, ((0, 4), (1, 4)))
    norm_gain = jnp.clip(1.0 + 0.18 * jax.random.normal(key_of[1], (D,), jnp.float32), 0.1, 1.9)
    key_weight = noise(key_of[2], (D, KVH * HD), D ** -0.5, 0.0625, ((1, 2),))
    value_weight = noise(key_of[3], (D, KVH * HD), D ** -0.5, 0.0625, ((1, 2),))
    prompt_lengths = touch_ends(jax.random.randint(key_of[4], (PROMPTS,), PLEN // 4, PLEN + 1), jax.random.fold_in(key_of[4], 1), PLEN // 4, PLEN).astype(jnp.int32)
    page_table = draw_page_table(jax.random.fold_in(key_of[9], 71), 0)
    request_slots = touch_ends(jax.random.randint(key_of[6], (REQS,), 0, PROMPTS), jax.random.fold_in(key_of[6], 1), 0, PROMPTS - 1).astype(jnp.int32)
    queries = draw_queries(jax.random.fold_in(key_of[9], 71), 0)
    new_kv = noise(key_of[8], (2, STEPS, REQS, KVH * HD), 1.0, 6.0, ((2, 16),))
    return dict(prompt_x=prompt_x, norm_gain=norm_gain, key_weight=key_weight, value_weight=value_weight, prompt_lengths=prompt_lengths, page_table=page_table, request_slots=request_slots, queries=queries, new_kv=new_kv)


rope_base = 500000.0
eps_norm = 1e-05

def rotate(values_in, positions, col_start, head_size):
    half_cols = values_in.shape[-1] // 2
    columns = col_start + 2 * jnp.arange(half_cols, dtype=jnp.int32)
    within = (columns % head_size).astype(jnp.float32)
    inverse = jnp.exp(-(within / head_size) * jnp.log(jnp.float32(rope_base)))
    angles = positions[..., None] * inverse
    cosine = jnp.cos(angles)
    sine_part = jnp.sin(angles)
    paired = values_in.reshape(values_in.shape[:-1] + (half_cols, 2))
    even_part = paired[..., 0]
    odd_part = paired[..., 1]
    turned = jnp.stack([even_part * cosine - odd_part * sine_part, even_part * sine_part + odd_part * cosine], -1)
    return turned.reshape(values_in.shape)

def widen(rows):
    split_rows = rows.reshape(PROMPTS, PLEN, KVH, 1, HD)
    copied = jnp.broadcast_to(split_rows, (PROMPTS, PLEN, KVH, REPL, HD))
    return copied.reshape(PROMPTS, PLEN, KV_COLS)

def round_weights(weights):
    return lax.optimization_barrier(weights.astype(jnp.bfloat16)).astype(jnp.float32)

def reference(prompt_x, norm_gain, key_weight, value_weight, prompt_lengths, page_table, request_slots, queries, new_kv):
    floated = prompt_x.astype(jnp.float32)
    square_mean = lax.optimization_barrier(jnp.mean(floated * floated, axis=-1, keepdims=True))
    normed = (floated * lax.rsqrt(square_mean + eps_norm) * norm_gain).astype(jnp.bfloat16)
    flat_rows = normed.reshape(PROMPTS * PLEN, D)
    key_rows = jnp.dot(flat_rows, key_weight, preferred_element_type=jnp.float32).reshape(PROMPTS, PLEN, KVH * HD)
    value_rows = jnp.dot(flat_rows, value_weight, preferred_element_type=jnp.float32).reshape(PROMPTS, PLEN, KVH * HD)
    value_rows = value_rows.astype(jnp.bfloat16)
    prompt_pos = jnp.arange(PLEN, dtype=jnp.int32).astype(jnp.float32)
    key_rows = rotate(key_rows, prompt_pos[None, :], 0, HD).astype(jnp.bfloat16)
    stacked = jnp.stack([widen(key_rows), widen(value_rows)], axis=1).reshape(PROMPTS, 2, BLOCKS, BLK, KV_COLS)
    blocks = stacked.transpose(0, 2, 1, 3, 4).reshape(PROMPTS * BLOCKS, 2, BLK, KV_COLS)
    paged_cache = jnp.zeros((PAGES, 2, BLK, KV_COLS), jnp.bfloat16).at[page_table.reshape(-1)].set(blocks)
    slot_len = prompt_lengths[request_slots]
    step_pos = (slot_len[None, :] + jnp.arange(STEPS, dtype=jnp.int32)[:, None]).astype(jnp.float32)
    rotated_q = rotate(queries.astype(jnp.float32), step_pos, 0, HD).astype(jnp.bfloat16)
    fresh_keys = rotate(new_kv[0].astype(jnp.float32), step_pos, 0, HD).astype(jnp.bfloat16)
    fresh_values = new_kv[1]
    group_size = QH // KVH
    score_scale = HD ** (-0.5)
    token_idx = jnp.arange(PLEN, dtype=jnp.int32)
    causal = jnp.arange(STEPS, dtype=jnp.int32)[None, :] <= jnp.arange(STEPS, dtype=jnp.int32)[:, None]
    highest = lax.Precision.HIGHEST

    def per_request(request):
        prompt = request_slots[request]
        length = prompt_lengths[prompt]
        cached_k = key_rows[prompt].astype(jnp.float32).reshape(PLEN, KVH, HD)
        cached_v = value_rows[prompt].astype(jnp.float32).reshape(PLEN, KVH, HD)
        query_rows = rotated_q[:, request].astype(jnp.float32).reshape(STEPS, KVH, group_size, HD)
        own_keys = fresh_keys[:, request].astype(jnp.float32).reshape(STEPS, KVH, HD)
        own_values = fresh_values[:, request].astype(jnp.float32).reshape(STEPS, KVH, HD)
        past_scores = jnp.einsum('tkgd,skd->tkgs', query_rows, cached_k, precision=highest) * score_scale
        recent_scores = jnp.einsum('tkgd,ukd->tkgu', query_rows, own_keys, precision=highest) * score_scale
        visible = (token_idx < length)[None, None, None, :]
        allowed = causal[:, None, None, :]
        row_peak = jnp.maximum(lax.optimization_barrier(jnp.max(jnp.where(visible, past_scores, -1e+30), axis=-1)), lax.optimization_barrier(jnp.max(jnp.where(allowed, recent_scores, -1e+30), axis=-1)))
        past_w = jnp.where(visible, jnp.exp(past_scores - row_peak[..., None]), 0.0)
        recent_w = jnp.where(allowed, jnp.exp(recent_scores - row_peak[..., None]), 0.0)
        row_total = lax.optimization_barrier(jnp.sum(past_w, axis=-1)) + lax.optimization_barrier(jnp.sum(recent_w, axis=-1))
        weighted = jnp.einsum('tkgs,skd->tkgd', round_weights(past_w), cached_v, precision=highest)
        weighted = weighted + jnp.einsum('tkgu,ukd->tkgd', round_weights(recent_w), own_values, precision=highest)
        return (weighted / row_total[..., None]).reshape(STEPS, QH * HD)
    attended = lax.map(per_request, jnp.arange(REQS, dtype=jnp.int32))
    return (attended.transpose(1, 0, 2).astype(jnp.bfloat16), paged_cache)
```

```python
import functools

import jax
import jax.numpy as jnp
from jax import lax
from jax.experimental import pallas as pl
from jax.experimental.pallas import tpu as pltpu
from jax.sharding import PartitionSpec as P

KVH = 8
HD = 128
ROPE_BASE = 500000.0
EPS = 1e-05
VMEM_BYTES = 60 * 1024 * 1024


def swapped(value, axis, bit):
    mask = 2**bit
    pairs = [(source, source ^ mask) for source in range(lax.axis_size(axis))]
    return lax.ppermute(value, axis, pairs)


def rope_tables(positions):
    column = jnp.arange(HD, dtype=jnp.int32)
    within = (column - column % 2).astype(jnp.float32)
    inverse = jnp.exp(-(within / HD) * jnp.log(jnp.float32(ROPE_BASE)))
    angles = positions[:, None] * inverse[None, :]
    sign = jnp.where(column % 2 == 0, -1.0, 1.0)
    return jnp.cos(angles), jnp.sin(angles) * sign[None, :]


def turn(block, cosine, sine):
    lane = lax.broadcasted_iota(jnp.int32, block.shape, 1)
    neighbour = jnp.where(
        lane % 2 == 0, pltpu.roll(block, HD - 1, 1), pltpu.roll(block, 1, 1)
    )
    return block * cosine + neighbour * sine


def project_kernel(
    x_ref, gain_ref, wk_ref, wv_ref, cos_ref, sin_ref, pages_ref, heads_ref, key_acc, value_acc
):
    rows, width = x_ref.shape
    head_width = wk_ref.shape[1]
    depth = min(1024, width)
    steps = width // depth

    def squares(i, partial):
        chunk = x_ref[:, pl.ds(pl.multiple_of(i * depth, depth), depth)].astype(jnp.float32)
        chunk = chunk * chunk
        for j in range(depth // HD):
            partial = partial + chunk[:, j * HD : (j + 1) * HD]
        return partial

    partial = lax.fori_loop(0, steps, squares, jnp.zeros((rows, HD), jnp.float32))
    scale = lax.rsqrt(jnp.sum(partial, axis=1, keepdims=True) / width + EPS)
    key_acc[...] = jnp.zeros_like(key_acc)
    value_acc[...] = jnp.zeros_like(value_acc)

    def multiply(i, carry):
        part = pl.ds(pl.multiple_of(i * depth, depth), depth)
        normed = (x_ref[:, part].astype(jnp.float32) * scale * gain_ref[:, part]).astype(
            jnp.bfloat16
        )
        key_acc[...] += jnp.dot(normed, wk_ref[part, :], preferred_element_type=jnp.float32)
        value_acc[...] += jnp.dot(normed, wv_ref[part, :], preferred_element_type=jnp.float32)
        return carry

    lax.fori_loop(0, steps, multiply, 0)
    page = pages_ref.shape[2]
    for h in range(head_width // HD):
        cols = slice(h * HD, (h + 1) * HD)
        keys = turn(key_acc[:, cols], cos_ref[...], sin_ref[...]).astype(jnp.bfloat16)
        values = value_acc[:, cols].astype(jnp.bfloat16)
        heads_ref[h, 0] = keys
        heads_ref[h, 1] = values
        for b in range(rows // page):
            pages_ref[b, 0, :, cols] = keys[b * page : (b + 1) * page]
            pages_ref[b, 1, :, cols] = values[b * page : (b + 1) * page]


def project(x, gain, wk, wv, cosine, sine, page):
    tokens, width = x.shape
    head_width = wk.shape[1]
    heads = head_width // HD
    rows = min(256, tokens)
    return pl.pallas_call(
        project_kernel,
        grid=(tokens // rows,),
        in_specs=[
            pl.BlockSpec((rows, width), lambda i: (i, 0)),
            pl.BlockSpec((1, width), lambda i: (0, 0)),
            pl.BlockSpec((width, head_width), lambda i: (0, 0), pipeline_mode=pl.Buffered(1)),
            pl.BlockSpec((width, head_width), lambda i: (0, 0), pipeline_mode=pl.Buffered(1)),
            pl.BlockSpec((rows, HD), lambda i: (i, 0)),
            pl.BlockSpec((rows, HD), lambda i: (i, 0)),
        ],
        out_specs=[
            pl.BlockSpec((rows // page, 2, page, head_width), lambda i: (i, 0, 0, 0)),
            pl.BlockSpec((heads, 2, rows, HD), lambda i: (0, 0, i, 0)),
        ],
        out_shape=[
            jax.ShapeDtypeStruct((tokens // page, 2, page, head_width), jnp.bfloat16),
            jax.ShapeDtypeStruct((heads, 2, tokens, HD), jnp.bfloat16),
        ],
        scratch_shapes=[
            pltpu.VMEM((rows, head_width), jnp.float32),
            pltpu.VMEM((rows, head_width), jnp.float32),
        ],
        compiler_params=pltpu.CompilerParams(vmem_limit_bytes=VMEM_BYTES),
        cost_estimate=pl.CostEstimate(
            flops=4 * tokens * width * head_width,
            bytes_accessed=2 * tokens * width + 4 * width * head_width,
            transcendentals=0,
        ),
        name="project",
    )(x, gain, wk, wv, cosine, sine)


MESH = pl.DeviceIdType.MESH


def place_of(seq_count):
    return lax.axis_index("rep") * seq_count + lax.axis_index("seq")


def greet(shards, seq_count):
    me = place_of(seq_count)
    barrier = pltpu.get_barrier_semaphore()
    for i in range(1, shards):
        peer = lax.rem(me + i, shards)
        pl.semaphore_signal(
            barrier,
            inc=1,
            device_id={"rep": peer // seq_count, "seq": lax.rem(peer, seq_count)},
            device_id_type=MESH,
        )
    pl.semaphore_wait(barrier, shards - 1)


BLOCK = 256


def stream_kernel(
    shards, seq_count, x_hbm, gain_ref, wk_hbm, wv_hbm, page_cos, page_sin, cell_cos, cell_sin,
    new_hbm, kv_out, new_out, xs, wide, acc, chunk, xsem, wsem, ksend, krecv, own_sem, nsend, nrecv,
    nown,
):
    tokens, width = x_hbm.shape
    heads = wk_hbm.shape[1] // HD
    blocks = tokens // BLOCK
    pairs = heads // 2
    page = cell_cos.shape[0]
    per_block = BLOCK // page
    me = place_of(seq_count)
    rep, seq = lax.axis_index("rep"), lax.axis_index("seq")
    order = [(heads // 2 + k) % heads for k in range(heads)]
    order = [o for o in order if o] + [0]
    head_of = [lax.rem(seq + o, heads) for o in order]

    def load_x(r):
        return pltpu.make_async_copy(x_hbm.at[pl.ds(r * BLOCK, BLOCK)], xs.at[pl.ds(r * BLOCK, BLOCK)], xsem.at[r])

    def load_w(k):
        cols = pl.ds(pl.multiple_of(head_of[k] * HD, HD), HD)
        at = (k % 2) * 2 * HD
        return [
            pltpu.make_async_copy(
                w.at[:, cols], wide.at[k // 2, :, pl.ds(at + j * HD, HD)], wsem.at[k, j]
            )
            for j, w in enumerate((wk_hbm, wv_hbm))
        ]

    load_x(0).start()
    for k in range(2):
        for copy in load_w(k):
            copy.start()
    for r in range(1, blocks):
        load_x(r).start()
    for k in range(2, heads):
        for copy in load_w(k):
            copy.start()

    greet(shards, seq_count)
    owned = new_hbm.shape[2]
    tp_head = lax.axis_index("tp") * heads

    def new_copy(i):
        peer = lax.rem(me + i, shards)
        peer_seq = lax.rem(peer, seq_count)
        cols = pl.ds(pl.multiple_of((tp_head + peer_seq) * HD, HD), HD)
        return pltpu.make_async_remote_copy(
            src_ref=new_hbm.at[:, :, :, cols],
            dst_ref=new_out.at[:, :, pl.ds(pl.multiple_of(me * owned, owned), owned), :],
            send_sem=nsend.at[i],
            recv_sem=nrecv.at[i],
            device_id={"rep": peer // seq_count, "seq": peer_seq},
            device_id_type=MESH,
        )

    for i in range(1, shards):
        new_copy(i).start()
    own_new = pltpu.make_async_copy(
        new_hbm.at[:, :, :, pl.ds(pl.multiple_of((tp_head + seq) * HD, HD), HD)],
        new_out.at[:, :, pl.ds(pl.multiple_of(me * owned, owned), owned), :],
        nown,
    )
    own_new.start()

    sub = min(64, BLOCK)

    def norm(r):
        for q in range(r * BLOCK, (r + 1) * BLOCK, sub):
            row = slice(q, q + sub)
            partial = jnp.zeros((sub, HD), jnp.float32)
            for j in range(0, width, 4 * HD):
                piece = xs[row, j : j + 4 * HD].astype(jnp.float32)
                piece = piece * piece
                for s in range(4):
                    partial = partial + piece[:, s * HD : (s + 1) * HD]
            scale = lax.rsqrt(jnp.sum(partial, axis=1, keepdims=True) / width + EPS)
            for j in range(0, width, 4 * HD):
                cols = slice(j, j + 4 * HD)
                xs[row, cols] = (
                    xs[row, cols].astype(jnp.float32) * scale * gain_ref[:, cols]
                ).astype(jnp.bfloat16)

    def kv_copy(k, r):
        part = pl.ds(r * per_block, per_block)
        return pltpu.make_async_remote_copy(
            src_ref=chunk.at[k, part],
            dst_ref=kv_out.at[seq, part],
            send_sem=ksend.at[k, r],
            recv_sem=krecv.at[k, r],
            device_id={"seq": head_of[k]},
            device_id_type=MESH,
        )

    def own_copy(r):
        part = pl.ds(r * per_block, per_block)
        return pltpu.make_async_copy(
            chunk.at[heads - 1, part], kv_out.at[seq, part], own_sem.at[r]
        )

    lane = lax.broadcasted_iota(jnp.int32, (page, HD), 1)
    even = lane % 2 == 0

    def finish(k, r, at):
        for b in range(per_block):
            rows = slice(b * page, (b + 1) * page)
            n = r * per_block + b
            base_cos, base_sin = page_cos[pl.ds(n, 1), :], page_sin[pl.ds(n, 1), :]
            cosine = base_cos * cell_cos[...] - base_sin * cell_sin[...]
            sine = base_sin * cell_cos[...] + base_cos * cell_sin[...]
            keys = acc[rows, at : at + HD]
            neighbour = jnp.where(even, -pltpu.roll(keys, HD - 1, 1), pltpu.roll(keys, 1, 1))
            chunk[k, n, 0] = (keys * cosine + neighbour * sine).astype(jnp.bfloat16)
            chunk[k, n, 1] = acc[rows, at + HD : at + 2 * HD].astype(jnp.bfloat16)
        if k == heads - 1:
            own_copy(r).start()
        else:
            kv_copy(k, r).start()

    load_x(0).wait()
    norm(0)
    for k in range(2):
        for copy in load_w(k):
            copy.wait()
    for r in range(blocks):
        if r + 1 < blocks:
            load_x(r + 1).wait()
        acc[...] = jnp.dot(
            xs[r * BLOCK : (r + 1) * BLOCK], wide[0], preferred_element_type=jnp.float32
        )
        if r + 1 < blocks:
            norm(r + 1)
        finish(0, r, 0)
        finish(1, r, 2 * HD)
    for pair in range(1, pairs):
        for k in (2 * pair, 2 * pair + 1):
            for copy in load_w(k):
                copy.wait()

        def rest(r, carry, pair=pair):
            rows = pl.ds(pl.multiple_of(r * BLOCK, BLOCK), BLOCK)
            acc[...] = jnp.dot(xs[rows], wide[pair], preferred_element_type=jnp.float32)
            finish(2 * pair, r, 0)
            finish(2 * pair + 1, r, 2 * HD)
            return carry

        lax.fori_loop(0, blocks, rest, 0)

    for r in range(blocks):
        own_copy(r).wait()
        for k in range(heads - 1):
            kv_copy(k, r).wait()
    own_new.wait()
    for i in range(1, shards):
        new_copy(i).wait()


def stream(x, gain, wk, wv, new_kv, page, shards, seq_count, seq_index):
    tokens, width = x.shape
    heads = wk.shape[1] // HD
    blocks = tokens // BLOCK
    pages = tokens // page
    steps, owned = new_kv.shape[1:3]
    first = (seq_index * pages + jnp.arange(pages, dtype=jnp.int32)) * page
    page_cos, page_sin = angle_tables(first.astype(jnp.float32))
    cell_cos, cell_sin = angle_tables(jnp.arange(page, dtype=jnp.int32).astype(jnp.float32))
    anywhere = pl.BlockSpec(memory_space=pl.ANY)
    here = pl.BlockSpec(memory_space=pltpu.VMEM)
    return pl.pallas_call(
        functools.partial(stream_kernel, shards, seq_count),
        in_specs=[anywhere, here, anywhere, anywhere, here, here, here, here, anywhere],
        out_specs=[anywhere, anywhere],
        out_shape=[
            jax.ShapeDtypeStruct((seq_count, pages, 2, page, HD), jnp.bfloat16),
            jax.ShapeDtypeStruct((2, steps, shards * owned, HD), jnp.bfloat16),
        ],
        scratch_shapes=[
            pltpu.VMEM((tokens, width), jnp.bfloat16),
            pltpu.VMEM((heads // 2, width, 4 * HD), jnp.bfloat16),
            pltpu.VMEM((BLOCK, 4 * HD), jnp.float32),
            pltpu.VMEM((heads, pages, 2, page, HD), jnp.bfloat16),
            pltpu.SemaphoreType.DMA((blocks,)),
            pltpu.SemaphoreType.DMA((heads, 2)),
            pltpu.SemaphoreType.DMA((heads, blocks)),
            pltpu.SemaphoreType.DMA((heads, blocks)),
            pltpu.SemaphoreType.DMA((blocks,)),
            pltpu.SemaphoreType.DMA((shards,)),
            pltpu.SemaphoreType.DMA((shards,)),
            pltpu.SemaphoreType.DMA(()),
        ],
        compiler_params=pltpu.CompilerParams(
            vmem_limit_bytes=VMEM_BYTES, collective_id=1, has_side_effects=True
        ),
        cost_estimate=pl.CostEstimate(
            flops=4 * tokens * width * heads * HD,
            bytes_accessed=2 * tokens * width + 4 * width * heads * HD,
            transcendentals=0,
        ),
        name="stream",
    )(x, gain, wk, wv, page_cos, page_sin, cell_cos, cell_sin, new_kv)


def angle_tables(positions):
    column = jnp.arange(HD, dtype=jnp.int32)
    within = (column - column % 2).astype(jnp.float32)
    inverse = jnp.exp(-(within / HD) * jnp.log(jnp.float32(ROPE_BASE)))
    angles = positions[:, None] * inverse[None, :]
    return jnp.cos(angles), jnp.sin(angles)


PIECES = 4


def exchange_kernel(
    cap, seq_count, rep_count, send_ref, pick_ref, kv_hbm, part_ref, pages_out, attn_out,
    kv, outgoing, turned, gathered, kv_sem, zsend, zrecv, psend, precv, psem, osend, orecv,
    *landing,
):
    shards = seq_count * rep_count
    blocks, _, page, _ = kv.shape
    half = page // 2
    pages = blocks // seq_count
    rep, seq = lax.axis_index("rep"), lax.axis_index("seq")
    me = place_of(seq_count)
    load = pltpu.make_async_copy(kv_hbm, kv, kv_sem)
    load.start()
    greet(shards, seq_count)
    load.wait()

    def rows_of(k):
        return k // 2, pl.ds((k % 2) * half, half)

    def z_copy(k, d):
        return pltpu.make_async_remote_copy(
            src_ref=outgoing.at[k, d - 1],
            dst_ref=landing[k].at[pl.ds((d - 1) * cap, cap)],
            send_sem=zsend.at[k, d - 1],
            recv_sem=zrecv.at[k, d - 1],
            device_id={"rep": rep ^ d},
            device_id_type=MESH,
        )

    far_first = sorted(range(1, rep_count), key=lambda d: -(d // 2 * 2))
    for k in range(PIECES):
        which, rows = rows_of(k)
        for d in far_first:

            def pack(j, carry, d=d, which=which, rows=rows, k=k):
                outgoing[k, d - 1, j] = kv[send_ref[d, j], which, rows, :]
                return carry

            lax.fori_loop(0, cap, pack, 0)
            z_copy(k, d).start()

        def keep(j, carry, which=which, rows=rows, k=k):
            landing[k][(rep_count - 1) * cap + j] = kv[send_ref[0, j], which, rows, :]
            return carry

        lax.fori_loop(0, landing[k].shape[0] - (rep_count - 1) * cap, keep, 0)

    def part_copy(i):
        peer = me ^ i
        return pltpu.make_async_remote_copy(
            src_ref=part_ref.at[peer],
            dst_ref=gathered.at[me],
            send_sem=osend.at[i],
            recv_sem=orecv.at[i],
            device_id={"rep": peer // seq_count, "seq": lax.rem(peer, seq_count)},
            device_id_type=MESH,
        )

    for i in range(shards - 1, 0, -1):
        part_copy(i).start()
    gathered[me] = part_ref[me]

    def p_copy(k, d):
        which, rows = rows_of(k)
        spot = pages_out.at[:, which, rows, pl.ds(pl.multiple_of(seq * HD, HD), HD)]
        if d == 0:
            return pltpu.make_async_copy(turned.at[k, 0], spot, psem.at[k])
        return pltpu.make_async_remote_copy(
            src_ref=turned.at[k, d],
            dst_ref=spot,
            send_sem=psend.at[k, d],
            recv_sem=precv.at[k, d],
            device_id={"seq": seq ^ d},
            device_id_type=MESH,
        )

    for k in range(PIECES):
        for d in far_first:
            z_copy(k, d).wait()
        for d in range(seq_count - 1, -1, -1):

            def sort(j, carry, d=d, k=k):
                turned[k, d, j] = landing[k][pick_ref[d, j]]
                return carry

            lax.fori_loop(0, pages, sort, 0)
            p_copy(k, d).start()

    for i in range(shards - 1, 0, -1):
        part_copy(i).wait()
    steps, owned, width = gathered.shape[1:]
    for s in range(seq_count):
        for t in range(steps):
            total = gathered[s, t]
            for z in range(1, rep_count):
                total = total + gathered[z * seq_count + s, t]
            attn_out[t, :, s * width : (s + 1) * width] = total

    for k in range(PIECES):
        for d in range(seq_count):
            p_copy(k, d).wait()


def exchange(cap, send, pick, kv, part, seq_count, rep_count, name, ident):
    _, pages, _, page, _ = kv.shape
    blocks = seq_count * pages
    shards, steps, owned, width = part.shape
    half = page // 2
    anywhere = pl.BlockSpec(memory_space=pl.ANY)
    here = pl.BlockSpec(memory_space=pltpu.VMEM)
    numbers = pl.BlockSpec(memory_space=pltpu.SMEM)
    landing = (rep_count - 1) * cap + send.shape[1]
    sems = pltpu.SemaphoreType.DMA
    return pl.pallas_call(
        functools.partial(exchange_kernel, cap, seq_count, rep_count),
        in_specs=[numbers, numbers, anywhere, here],
        out_specs=[anywhere, here],
        out_shape=[
            jax.ShapeDtypeStruct((pages, 2, page, seq_count * HD), jnp.bfloat16),
            jax.ShapeDtypeStruct((steps, owned, seq_count * width), jnp.bfloat16),
        ],
        scratch_shapes=[
            pltpu.VMEM((blocks, 2, page, HD), jnp.bfloat16),
            pltpu.VMEM((PIECES, rep_count - 1, cap, half, HD), jnp.bfloat16),
            pltpu.VMEM((PIECES, seq_count, pages, half, HD), jnp.bfloat16),
            pltpu.VMEM((shards, steps, owned, width), jnp.bfloat16),
            sems(()),
            sems((PIECES, rep_count)),
            sems((PIECES, rep_count)),
            sems((PIECES, seq_count)),
            sems((PIECES, seq_count)),
            sems((PIECES,)),
            sems((shards,)),
            sems((shards,)),
        ]
        + [pltpu.VMEM((landing, half, HD), jnp.bfloat16)] * PIECES,
        compiler_params=pltpu.CompilerParams(
            vmem_limit_bytes=VMEM_BYTES, collective_id=ident, has_side_effects=True
        ),
        cost_estimate=pl.CostEstimate(
            flops=1, bytes_accessed=8 * 1024 * 1024, transcendentals=0
        ),
        name=name,
    )(send, pick, kv.reshape(blocks, 2, page, HD), part)


def routes(page_table, cap, rep_index, seq_index, rep_count, seq_count):
    prompts, blocks = page_table.shape
    pages = blocks // seq_count
    most = blocks // 2
    plane = page_table // (pages * seq_count)
    block = jnp.arange(blocks, dtype=jnp.int32)
    same = (plane[:, :, None] == plane[:, None, :]) & (block[None, :, None] > block[None, None, :])
    rank = jnp.sum(same.astype(jnp.int32), axis=2)
    apart = jnp.arange(rep_count, dtype=jnp.int32)
    slot = jnp.arange(most, dtype=jnp.int32)
    own_plane = lax.dynamic_index_in_dim(plane, rep_index, 0, keepdims=False)
    own_rank = lax.dynamic_index_in_dim(rank, rep_index, 0, keepdims=False)
    match = (own_plane[None, None, :] == (rep_index ^ apart)[:, None, None]) & (
        own_rank[None, None, :] == slot[None, :, None]
    )
    send = jnp.sum(match.astype(jnp.int32) * block[None, None, :], axis=2)
    away = jnp.arange(prompts, dtype=jnp.int32) ^ rep_index
    origin = jnp.where(away == 0, (rep_count - 1), away - 1)
    spot = (origin[:, None] * cap + rank).reshape(-1)
    shard = rep_index * seq_count + (seq_index ^ jnp.arange(seq_count, dtype=jnp.int32))
    wanted = shard[:, None] * pages + jnp.arange(pages, dtype=jnp.int32)[None, :]
    found = (wanted[:, :, None] == page_table.reshape(-1)[None, None, :]).astype(jnp.int32)
    pick = jnp.sum(found * spot[None, None, :], axis=2)
    return send, pick


def busiest(page_table, rep_count, seq_count):
    prompts, blocks = page_table.shape
    plane = page_table // blocks
    counts = jnp.sum(
        (plane[:, None, :] == jnp.arange(rep_count, dtype=jnp.int32)[None, :, None]).astype(
            jnp.int32
        ),
        axis=2,
    )
    other = jnp.arange(prompts, dtype=jnp.int32)[:, None] != jnp.arange(rep_count)[None, :]
    return jnp.max(jnp.where(other, counts, 0))


TIGHT = 12


ROWS = 16


def attend_kernel(
    scalars, q_ref, new_ref, kv_ref, slot_row_ref, slot_col_ref, cos_ref, sin_ref, out_ref,
    rotated, acc, done,
):
    prompt, length = scalars[1], scalars[2]
    steps, requests, width = q_ref.shape
    group = width // HD
    paged = len(kv_ref.shape) == 5
    span = kv_ref.shape[1] * kv_ref.shape[3] if paged else kv_ref.shape[2]

    def source(c, which):
        if paged:
            return kv_ref[c, :, which].reshape(span, HD)
        return kv_ref[c, which]

    rows = steps * group * ROWS
    score_scale = HD ** (-0.5)

    hit_row = slot_row_ref[...] == prompt
    hit_col = slot_col_ref[...] == prompt
    square = (requests, requests)
    first = lax.broadcasted_iota(jnp.int32, square, 0)
    second = lax.broadcasted_iota(jnp.int32, square, 1)
    rank_row = jnp.sum(
        jnp.where(hit_col & (first < second), 1.0, 0.0), axis=0, keepdims=True
    ).astype(jnp.int32)
    rank_col = jnp.sum(
        jnp.where(hit_row & (second < first), 1.0, 0.0), axis=1, keepdims=True
    ).astype(jnp.int32)
    count = jnp.sum(jnp.where(hit_row, 1.0, 0.0)).astype(jnp.int32)
    done[...] = jnp.zeros_like(done)
    chunks = (length + span - 1) // span

    def tile(k, carry):
        want = k * ROWS + lax.broadcasted_iota(jnp.int32, (ROWS, requests), 0)
        pick = jnp.where((rank_row == want) & hit_row, 1.0, 0.0).astype(jnp.bfloat16)
        fresh_keys, fresh_values = [], []
        for t in range(steps):
            cosine, sine = cos_ref[t : t + 1, :], sin_ref[t : t + 1, :]
            picked = jnp.dot(pick, q_ref[t], preferred_element_type=jnp.float32)
            for g in range(group):
                head = turn(picked[:, g * HD : (g + 1) * HD], cosine, sine)
                at = (t * group + g) * ROWS
                rotated[at : at + ROWS, :] = head.astype(jnp.bfloat16)
            picked = jnp.dot(pick, new_ref[0, t], preferred_element_type=jnp.float32)
            fresh_keys.append(turn(picked, cosine, sine).astype(jnp.bfloat16))
            picked = jnp.dot(pick, new_ref[1, t], preferred_element_type=jnp.float32)
            fresh_values.append(picked.astype(jnp.bfloat16))
        fresh_keys = jnp.concatenate(fresh_keys, axis=0)
        fresh_values = jnp.concatenate(fresh_values, axis=0)
        scores = score_scale * lax.dot_general(
            rotated[...], fresh_keys, (((1,), (1,)), ((), ())), preferred_element_type=jnp.float32
        )
        row = lax.broadcasted_iota(jnp.int32, scores.shape, 0)
        column = lax.broadcasted_iota(jnp.int32, scores.shape, 1)
        allowed = (row % ROWS == column % ROWS) & (column // ROWS <= row // (group * ROWS))
        peak = jnp.max(jnp.where(allowed, scores, -1e30), axis=1, keepdims=True)
        weights = jnp.where(allowed, jnp.exp(scores - peak), 0.0)
        total = jnp.sum(weights, axis=1, keepdims=True)
        acc[...] = jnp.dot(
            weights.astype(jnp.bfloat16), fresh_values, preferred_element_type=jnp.float32
        )

        def chunk(c, state):
            peak, total = state
            scores = score_scale * lax.dot_general(
                rotated[...], source(c, 0), (((1,), (1,)), ((), ())),
                preferred_element_type=jnp.float32,
            )
            position = c * span + lax.broadcasted_iota(jnp.int32, (1, span), 1)
            scores = jnp.where(position < length, scores, -1e30)
            new_peak = jnp.maximum(peak, jnp.max(scores, axis=1, keepdims=True))
            weights = jnp.exp(scores - new_peak)
            factor = jnp.exp(peak - new_peak)
            total = total * factor + jnp.sum(weights, axis=1, keepdims=True)
            acc[...] = acc[...] * factor + jnp.dot(
                weights.astype(jnp.bfloat16), source(c, 1), preferred_element_type=jnp.float32
            )
            return new_peak, total

        peak, total = lax.fori_loop(0, chunks, chunk, (peak, total))
        result = (acc[...] / total).astype(jnp.bfloat16)
        here = pl.ds(pl.multiple_of(k * ROWS, ROWS), ROWS)
        for t in range(steps):
            for g in range(group):
                at = (t * group + g) * ROWS
                done[t, here, g * HD : (g + 1) * HD] = result[at : at + ROWS]
        return carry

    lax.fori_loop(0, (count + ROWS - 1) // ROWS, tile, 0)
    place = jnp.where((rank_col == second) & hit_col, 1.0, 0.0).astype(jnp.bfloat16)
    owned = out_ref.shape[2]
    for t in range(steps):
        spread = jnp.dot(place, done[t], preferred_element_type=jnp.float32)
        for d in range(out_ref.shape[0]):
            out_ref[d, t] = spread[d * owned : (d + 1) * owned].astype(jnp.bfloat16)


def attend(scalars, queries, new_kv, kv, slots, cosine, sine, shards, seq_count, fresh_split):
    steps, requests, query_width = queries.shape
    width = query_width // seq_count
    rows = steps * (width // HD) * ROWS
    padded = -(-requests // ROWS) * ROWS
    whole = lambda shape: pl.BlockSpec(shape, lambda i, s: (0,) * len(shape))
    fresh_index = (lambda i, s: (0, 0, 0, s[0])) if fresh_split else (lambda i, s: (0, 0, 0, 0))
    return pl.pallas_call(
        attend_kernel,
        grid_spec=pltpu.PrefetchScalarGridSpec(
            num_scalar_prefetch=1,
            grid=(1,),
            in_specs=[
                pl.BlockSpec((steps, requests, width), lambda i, s: (0, 0, s[0])),
                pl.BlockSpec((2, steps, requests, HD), fresh_index),
                whole(kv.shape),
                whole((1, requests)),
                whole((requests, 1)),
                whole(cosine.shape),
                whole(sine.shape),
            ],
            out_specs=whole((shards, steps, requests // shards, width)),
            scratch_shapes=[
                pltpu.VMEM((rows, HD), jnp.bfloat16),
                pltpu.VMEM((rows, HD), jnp.float32),
                pltpu.VMEM((steps, padded, width), jnp.bfloat16),
            ],
        ),
        out_shape=jax.ShapeDtypeStruct(
            (shards, steps, requests // shards, width), jnp.bfloat16
        ),
        compiler_params=pltpu.CompilerParams(vmem_limit_bytes=VMEM_BYTES),
        cost_estimate=pl.CostEstimate(
            flops=steps * requests * width * kv.size // (2 * HD),
            bytes_accessed=8 * 1024 * 1024,
            transcendentals=0,
        ),
        name="attend",
    )(scalars, queries, new_kv, kv, slots[None, :], slots[:, None], cosine, sine)


def fast_body(
    prompt_x, norm_gain, key_weight, value_weight, prompt_lengths, page_table, request_slots,
    queries, new_kv,
):
    seq_count = lax.axis_size("seq")
    rep_count = lax.axis_size("rep")
    rep_index = lax.axis_index("rep")
    seq_index = lax.axis_index("seq")
    shards = rep_count * seq_count
    blocks = page_table.shape[1]
    pages = blocks // seq_count
    page = prompt_x.shape[1] // pages
    kv, all_new = stream(
        prompt_x[0], norm_gain[None, :], key_weight, value_weight, new_kv, page, shards,
        seq_count, seq_index,
    )
    own_length = lax.dynamic_index_in_dim(prompt_lengths, rep_index, 0, keepdims=False)
    steps = queries.shape[0]
    step_pos = (own_length + jnp.arange(steps, dtype=jnp.int32)).astype(jnp.float32)
    step_cos, step_sin = rope_tables(step_pos)
    scalars = jnp.stack([seq_index, rep_index, own_length]).astype(jnp.int32)
    part = attend(
        scalars, queries, all_new, kv, request_slots, step_cos, step_sin, shards, seq_count, False
    )
    most = blocks // 2

    def tight(args):
        send, pick = routes(page_table, TIGHT, rep_index, seq_index, rep_count, seq_count)
        return exchange(TIGHT, send, pick, *args, seq_count, rep_count, "exchange", 2)

    def full(args):
        send, pick = routes(page_table, most, rep_index, seq_index, rep_count, seq_count)
        return exchange(most, send, pick, *args, seq_count, rep_count, "exchange_full", 3)

    fits = busiest(page_table, rep_count, seq_count) <= TIGHT
    paged_cache, attention = lax.cond(fits, tight, full, (kv, part))
    return (attention, paged_cache)


def quick(prompt_x, key_weight, page_table, new_kv):
    seq_count, rep_count = lax.axis_size("seq"), lax.axis_size("rep")
    heads = key_weight.shape[1] // HD
    powers = all(n & (n - 1) == 0 for n in (seq_count, rep_count))
    return (
        powers
        and key_weight.shape[1] % HD == 0
        and heads == seq_count
        and heads % 2 == 0
        and lax.axis_size("tp") * heads == KVH
        and prompt_x.shape[0] == 1
        and page_table.shape[0] == rep_count
        and prompt_x.shape[1] % BLOCK == 0
    )


def body(
    prompt_x,
    norm_gain,
    key_weight,
    value_weight,
    prompt_lengths,
    page_table,
    request_slots,
    queries,
    new_kv,
):
    seq_count = lax.axis_size("seq")
    rep_count = lax.axis_size("rep")
    tp_count = lax.axis_size("tp")
    rep_index = lax.axis_index("rep")
    seq_index = lax.axis_index("seq")
    tp_index = lax.axis_index("tp")
    shard_index = rep_index * seq_count + seq_index
    shard_count = rep_count * seq_count
    tokens = prompt_x.shape[1]
    if quick(prompt_x, key_weight, page_table, new_kv):
        return fast_body(
            prompt_x, norm_gain, key_weight, value_weight, prompt_lengths, page_table,
            request_slots, queries, new_kv,
        )
    prompts, blocks_per_prompt = page_table.shape
    pages_here = blocks_per_prompt // seq_count
    page = tokens // pages_here
    copies = max(1, tp_count // KVH)
    key_cols, value_cols = key_weight, value_weight
    if tp_count > KVH:
        other_key, other_value = swapped((key_weight, value_weight), "tp", 0)
        low_half = tp_index % 2 == 0
        key_cols = jnp.where(
            low_half,
            jnp.concatenate([key_weight, other_key], 1),
            jnp.concatenate([other_key, key_weight], 1),
        )
        value_cols = jnp.where(
            low_half,
            jnp.concatenate([value_weight, other_value], 1),
            jnp.concatenate([other_value, value_weight], 1),
        )
    head_width = key_cols.shape[1]
    heads_here = head_width // HD
    head_start = tp_index * heads_here // copies

    own_new = lax.dynamic_slice_in_dim(new_kv, head_start * HD, head_width, 3)
    all_new = lax.all_gather(own_new, ("rep", "seq"), axis=2, tiled=True)

    token_pos = (seq_index * tokens + jnp.arange(tokens, dtype=jnp.int32)).astype(jnp.float32)
    cosine, sine = rope_tables(token_pos)
    pages, heads = project(
        prompt_x[0], norm_gain[None, :], key_cols, value_cols, cosine, sine, page
    )

    by_head = heads_here == seq_count
    if by_head:
        kv = lax.all_to_all(heads, "seq", split_axis=0, concat_axis=0, tiled=True)
    else:
        kv = lax.all_gather(heads, "seq", axis=0, tiled=True)

    own_pages = lax.dynamic_slice(page_table, (rep_index, seq_index * pages_here), (1, pages_here))[0]
    hits = (
        own_pages[None, :] // pages_here == jnp.arange(shard_count, dtype=jnp.int32)[:, None]
    ).astype(jnp.int32)
    chosen = jnp.sum(hits * jnp.arange(pages_here, dtype=jnp.int32)[None, :], axis=1)
    outgoing = jnp.take(pages, chosen, axis=0, mode="clip")
    arrived = lax.all_to_all(outgoing, ("rep", "seq"), split_axis=0, concat_axis=0, tiled=True)
    page_ids = shard_index * pages_here + jnp.arange(pages_here, dtype=jnp.int32)
    flat_source = jnp.arange(prompts * blocks_per_prompt, dtype=jnp.int32) // pages_here
    matches = (page_table.reshape(-1)[None, :] == page_ids[:, None]).astype(jnp.int32)
    sources = jnp.sum(matches * flat_source[None, :], axis=1)
    paged_cache = jnp.take(arrived, sources, axis=0, mode="clip")

    own_length = lax.dynamic_index_in_dim(prompt_lengths, rep_index, 0, keepdims=False)
    steps = queries.shape[0]
    step_pos = (own_length + jnp.arange(steps, dtype=jnp.int32)).astype(jnp.float32)
    step_cos, step_sin = rope_tables(step_pos)
    scalars = jnp.stack([seq_index, rep_index, own_length]).astype(jnp.int32)
    partial = attend(
        scalars, queries, all_new, kv, request_slots, step_cos, step_sin, shard_count, seq_count,
        by_head,
    )
    owned = lax.all_to_all(partial, ("rep", "seq"), split_axis=0, concat_axis=0, tiled=True)
    attention = jnp.concatenate(
        [
            functools.reduce(
                jnp.add, [owned[r * seq_count + s] for r in range(rep_count)]
            )
            for s in range(seq_count)
        ],
        axis=-1,
    )
    return (attention, paged_cache)


def solution(mesh):
    in_specs = (
        P("rep", "seq", None),
        P(),
        P(None, "tp"),
        P(None, "tp"),
        P(),
        P(),
        P(),
        P(None, None, "tp"),
        P(None, None, ("rep", "seq"), None),
    )
    out_specs = (P(None, ("rep", "seq"), "tp"), P(("rep", "seq"), None, None, "tp"))
    return jax.shard_map(body, mesh=mesh, in_specs=in_specs, out_specs=out_specs, check_vma=False)
```

```python
import functools

import jax
import jax.numpy as jnp
from jax import lax
from jax.experimental import pallas as pl
from jax.experimental.pallas import tpu as pltpu
from jax.sharding import PartitionSpec as P

KVH = 8
HD = 128
ROPE_BASE = 500000.0
EPS = 1e-05
VMEM_BYTES = 60 * 1024 * 1024


def swapped(value, axis, bit):
    mask = 2**bit
    pairs = [(source, source ^ mask) for source in range(lax.axis_size(axis))]
    return lax.ppermute(value, axis, pairs)


def rope_tables(positions):
    column = jnp.arange(HD, dtype=jnp.int32)
    within = (column - column % 2).astype(jnp.float32)
    inverse = jnp.exp(-(within / HD) * jnp.log(jnp.float32(ROPE_BASE)))
    angles = positions[:, None] * inverse[None, :]
    sign = jnp.where(column % 2 == 0, -1.0, 1.0)
    return jnp.cos(angles), jnp.sin(angles) * sign[None, :]


def turn(block, cosine, sine):
    lane = lax.broadcasted_iota(jnp.int32, block.shape, 1)
    neighbour = jnp.where(
        lane % 2 == 0, pltpu.roll(block, HD - 1, 1), pltpu.roll(block, 1, 1)
    )
    return block * cosine + neighbour * sine


def project_kernel(
    x_ref, gain_ref, wk_ref, wv_ref, cos_ref, sin_ref, pages_ref, heads_ref, key_acc, value_acc
):
    rows, width = x_ref.shape
    head_width = wk_ref.shape[1]
    depth = min(1024, width)
    steps = width // depth

    def squares(i, partial):
        chunk = x_ref[:, pl.ds(pl.multiple_of(i * depth, depth), depth)].astype(jnp.float32)
        chunk = chunk * chunk
        for j in range(depth // HD):
            partial = partial + chunk[:, j * HD : (j + 1) * HD]
        return partial

    partial = lax.fori_loop(0, steps, squares, jnp.zeros((rows, HD), jnp.float32))
    scale = lax.rsqrt(jnp.sum(partial, axis=1, keepdims=True) / width + EPS)
    key_acc[...] = jnp.zeros_like(key_acc)
    value_acc[...] = jnp.zeros_like(value_acc)

    def multiply(i, carry):
        part = pl.ds(pl.multiple_of(i * depth, depth), depth)
        normed = (x_ref[:, part].astype(jnp.float32) * scale * gain_ref[:, part]).astype(
            jnp.bfloat16
        )
        key_acc[...] += jnp.dot(normed, wk_ref[part, :], preferred_element_type=jnp.float32)
        value_acc[...] += jnp.dot(normed, wv_ref[part, :], preferred_element_type=jnp.float32)
        return carry

    lax.fori_loop(0, steps, multiply, 0)
    page = pages_ref.shape[2]
    for h in range(head_width // HD):
        cols = slice(h * HD, (h + 1) * HD)
        keys = turn(key_acc[:, cols], cos_ref[...], sin_ref[...]).astype(jnp.bfloat16)
        values = value_acc[:, cols].astype(jnp.bfloat16)
        heads_ref[h, 0] = keys
        heads_ref[h, 1] = values
        for b in range(rows // page):
            pages_ref[b, 0, :, cols] = keys[b * page : (b + 1) * page]
            pages_ref[b, 1, :, cols] = values[b * page : (b + 1) * page]


def project(x, gain, wk, wv, cosine, sine, page):
    tokens, width = x.shape
    head_width = wk.shape[1]
    heads = head_width // HD
    rows = min(256, tokens)
    return pl.pallas_call(
        project_kernel,
        grid=(tokens // rows,),
        in_specs=[
            pl.BlockSpec((rows, width), lambda i: (i, 0)),
            pl.BlockSpec((1, width), lambda i: (0, 0)),
            pl.BlockSpec((width, head_width), lambda i: (0, 0), pipeline_mode=pl.Buffered(1)),
            pl.BlockSpec((width, head_width), lambda i: (0, 0), pipeline_mode=pl.Buffered(1)),
            pl.BlockSpec((rows, HD), lambda i: (i, 0)),
            pl.BlockSpec((rows, HD), lambda i: (i, 0)),
        ],
        out_specs=[
            pl.BlockSpec((rows // page, 2, page, head_width), lambda i: (i, 0, 0, 0)),
            pl.BlockSpec((heads, 2, rows, HD), lambda i: (0, 0, i, 0)),
        ],
        out_shape=[
            jax.ShapeDtypeStruct((tokens // page, 2, page, head_width), jnp.bfloat16),
            jax.ShapeDtypeStruct((heads, 2, tokens, HD), jnp.bfloat16),
        ],
        scratch_shapes=[
            pltpu.VMEM((rows, head_width), jnp.float32),
            pltpu.VMEM((rows, head_width), jnp.float32),
        ],
        compiler_params=pltpu.CompilerParams(vmem_limit_bytes=VMEM_BYTES),
        cost_estimate=pl.CostEstimate(
            flops=4 * tokens * width * head_width,
            bytes_accessed=2 * tokens * width + 4 * width * head_width,
            transcendentals=0,
        ),
        name="project",
    )(x, gain, wk, wv, cosine, sine)


MESH = pl.DeviceIdType.MESH


def place_of(seq_count):
    return lax.axis_index("rep") * seq_count + lax.axis_index("seq")


def greet(shards, seq_count):
    me = place_of(seq_count)
    barrier = pltpu.get_barrier_semaphore()
    for i in range(1, shards):
        peer = lax.rem(me + i, shards)
        pl.semaphore_signal(
            barrier,
            inc=1,
            device_id={"rep": peer // seq_count, "seq": lax.rem(peer, seq_count)},
            device_id_type=MESH,
        )
    pl.semaphore_wait(barrier, shards - 1)


BLOCK = 256
ROWS = 16


def stream_kernel(
    shards, seq_count, page, x_hbm, gain_ref, wk_hbm, wv_hbm, cos_ref, sin_ref,
    new_hbm, kv_out, new_out, xs, wide, acc, chunk, xsem, wsem, ksend, krecv, own_sem, nsend, nrecv,
    nown,
):
    tokens, width = x_hbm.shape
    heads = wk_hbm.shape[1] // HD
    blocks = tokens // BLOCK
    pairs = heads // 2
    per_block = BLOCK // page
    me = place_of(seq_count)
    rep, seq = lax.axis_index("rep"), lax.axis_index("seq")
    order = [(heads // 2 + k) % heads for k in range(heads)]
    order = [o for o in order if o] + [0]
    head_of = [lax.rem(seq + o, heads) for o in order]

    def load_x(r):
        return pltpu.make_async_copy(x_hbm.at[pl.ds(r * BLOCK, BLOCK)], xs.at[pl.ds(r * BLOCK, BLOCK)], xsem.at[r])

    def load_w(k):
        cols = pl.ds(pl.multiple_of(head_of[k] * HD, HD), HD)
        at = (k % 2) * 2 * HD
        return [
            pltpu.make_async_copy(
                w.at[:, cols], wide.at[k // 2, :, pl.ds(at + j * HD, HD)], wsem.at[k, j]
            )
            for j, w in enumerate((wk_hbm, wv_hbm))
        ]

    load_x(0).start()
    for k in range(2):
        for copy in load_w(k):
            copy.start()
    for r in range(1, blocks):
        load_x(r).start()
    for k in range(2, heads):
        for copy in load_w(k):
            copy.start()

    greet(shards, seq_count)
    owned = new_hbm.shape[2]
    tp_head = lax.axis_index("tp") * heads

    def new_copy(i):
        peer = lax.rem(me + i, shards)
        peer_seq = lax.rem(peer, seq_count)
        cols = pl.ds(pl.multiple_of((tp_head + peer_seq) * HD, HD), HD)
        return pltpu.make_async_remote_copy(
            src_ref=new_hbm.at[:, :, :, cols],
            dst_ref=new_out.at[:, :, pl.ds(pl.multiple_of(me * owned, owned), owned), :],
            send_sem=nsend.at[i],
            recv_sem=nrecv.at[i],
            device_id={"rep": peer // seq_count, "seq": peer_seq},
            device_id_type=MESH,
        )

    for i in range(1, shards):
        new_copy(i).start()
    own_new = pltpu.make_async_copy(
        new_hbm.at[:, :, :, pl.ds(pl.multiple_of((tp_head + seq) * HD, HD), HD)],
        new_out.at[:, :, pl.ds(pl.multiple_of(me * owned, owned), owned), :],
        nown,
    )
    own_new.start()

    sub = min(64, BLOCK)

    def norm(r):
        for q in range(r * BLOCK, (r + 1) * BLOCK, sub):
            row = slice(q, q + sub)
            partial = jnp.zeros((sub, HD), jnp.float32)
            for j in range(0, width, 4 * HD):
                piece = xs[row, j : j + 4 * HD].astype(jnp.float32)
                piece = piece * piece
                for s in range(4):
                    partial = partial + piece[:, s * HD : (s + 1) * HD]
            scale = lax.rsqrt(jnp.sum(partial, axis=1, keepdims=True) / width + EPS)
            for j in range(0, width, 4 * HD):
                cols = slice(j, j + 4 * HD)
                xs[row, cols] = (
                    xs[row, cols].astype(jnp.float32) * scale * gain_ref[:, cols]
                ).astype(jnp.bfloat16)

    def kv_copy(k, r):
        part = pl.ds(r * per_block, per_block)
        return pltpu.make_async_remote_copy(
            src_ref=chunk.at[k, part],
            dst_ref=kv_out.at[seq, part],
            send_sem=ksend.at[k, r],
            recv_sem=krecv.at[k, r],
            device_id={"seq": head_of[k]},
            device_id_type=MESH,
        )

    def own_copy(r):
        part = pl.ds(r * per_block, per_block)
        return pltpu.make_async_copy(
            chunk.at[heads - 1, part], kv_out.at[seq, part], own_sem.at[r]
        )

    lane = lax.broadcasted_iota(jnp.int32, (page, HD), 1)
    even = lane % 2 == 0

    def finish(k, r, at):
        for b in range(per_block):
            rows = slice(b * page, (b + 1) * page)
            n = r * per_block + b
            base_cos, base_sin = cos_ref[pl.ds(page + n, 1), :], sin_ref[pl.ds(page + n, 1), :]
            cell_cos, cell_sin = cos_ref[:page, :], sin_ref[:page, :]
            cosine = base_cos * cell_cos - base_sin * cell_sin
            sine = base_sin * cell_cos + base_cos * cell_sin
            keys = acc[rows, at : at + HD]
            neighbour = jnp.where(even, -pltpu.roll(keys, HD - 1, 1), pltpu.roll(keys, 1, 1))
            chunk[k, n, 0] = (keys * cosine + neighbour * sine).astype(jnp.bfloat16)
            chunk[k, n, 1] = acc[rows, at + HD : at + 2 * HD].astype(jnp.bfloat16)
        if k == heads - 1:
            own_copy(r).start()
        else:
            kv_copy(k, r).start()

    load_x(0).wait()
    norm(0)
    for k in range(2):
        for copy in load_w(k):
            copy.wait()
    for r in range(blocks):
        if r + 1 < blocks:
            load_x(r + 1).wait()
        acc[...] = jnp.dot(
            xs[r * BLOCK : (r + 1) * BLOCK], wide[0], preferred_element_type=jnp.float32
        )
        if r + 1 < blocks:
            norm(r + 1)
        finish(0, r, 0)
        finish(1, r, 2 * HD)
    for pair in range(1, pairs):
        for k in (2 * pair, 2 * pair + 1):
            for copy in load_w(k):
                copy.wait()

        def rest(r, carry, pair=pair):
            rows = pl.ds(pl.multiple_of(r * BLOCK, BLOCK), BLOCK)
            acc[...] = jnp.dot(xs[rows], wide[pair], preferred_element_type=jnp.float32)
            finish(2 * pair, r, 0)
            finish(2 * pair + 1, r, 2 * HD)
            return carry

        lax.fori_loop(0, blocks, rest, 0)

    for r in range(blocks):
        own_copy(r).wait()
        for k in range(heads - 1):
            kv_copy(k, r).wait()
    own_new.wait()
    for i in range(1, shards):
        new_copy(i).wait()


def stream(x, gain, wk, wv, new_kv, cosine, sine, page, shards, seq_count):
    tokens, width = x.shape
    heads = wk.shape[1] // HD
    blocks = tokens // BLOCK
    pages = tokens // page
    steps, owned = new_kv.shape[1:3]
    anywhere = pl.BlockSpec(memory_space=pl.ANY)
    here = pl.BlockSpec(memory_space=pltpu.VMEM)
    return pl.pallas_call(
        functools.partial(stream_kernel, shards, seq_count, page),
        in_specs=[anywhere, here, anywhere, anywhere, here, here, anywhere],
        out_specs=[anywhere, anywhere],
        out_shape=[
            jax.ShapeDtypeStruct((seq_count, pages, 2, page, HD), jnp.bfloat16),
            jax.ShapeDtypeStruct((2, steps, shards * owned, HD), jnp.bfloat16),
        ],
        scratch_shapes=[
            pltpu.VMEM((tokens, width), jnp.bfloat16),
            pltpu.VMEM((heads // 2, width, 4 * HD), jnp.bfloat16),
            pltpu.VMEM((BLOCK, 4 * HD), jnp.float32),
            pltpu.VMEM((heads, pages, 2, page, HD), jnp.bfloat16),
            pltpu.SemaphoreType.DMA((blocks,)),
            pltpu.SemaphoreType.DMA((heads, 2)),
            pltpu.SemaphoreType.DMA((heads, blocks)),
            pltpu.SemaphoreType.DMA((heads, blocks)),
            pltpu.SemaphoreType.DMA((blocks,)),
            pltpu.SemaphoreType.DMA((shards,)),
            pltpu.SemaphoreType.DMA((shards,)),
            pltpu.SemaphoreType.DMA(()),
        ],
        compiler_params=pltpu.CompilerParams(
            vmem_limit_bytes=VMEM_BYTES, collective_id=1, has_side_effects=True
        ),
        cost_estimate=pl.CostEstimate(
            flops=4 * tokens * width * heads * HD,
            bytes_accessed=2 * tokens * width + 4 * width * heads * HD,
            transcendentals=0,
        ),
        name="stream",
    )(x, gain, wk, wv, cosine, sine, new_kv)


def angle_tables(positions):
    column = jnp.arange(HD, dtype=jnp.int32)
    within = (column - column % 2).astype(jnp.float32)
    inverse = jnp.exp(-(within / HD) * jnp.log(jnp.float32(ROPE_BASE)))
    angles = positions[:, None] * inverse[None, :]
    return jnp.cos(angles), jnp.sin(angles)


PIECES = 4


def exchange_kernel(
    cap, seats, tiles, seq_count, rep_count, send_ref, pick_ref, length_ref, slot_ref, seat_ref,
    cos_ref, sin_ref, kv_hbm, q_hbm, new_hbm, pages_out, attn_out,
    kv, outgoing, turned, queries, fresh, rotated, acc, done, parts, landed, owned_out,
    load_sem, zsend, zrecv, psend, precv, psem, osend, orecv, asend, arecv, asem, *landing,
):
    shards = seq_count * rep_count
    blocks, _, page, _ = kv.shape
    half = page // 2
    pages = blocks // seq_count
    steps, requests, width = queries.shape
    group = width // HD
    rep, seq = lax.axis_index("rep"), lax.axis_index("seq")
    loads = [
        pltpu.make_async_copy(kv_hbm, kv, load_sem.at[0]),
        pltpu.make_async_copy(
            q_hbm.at[:, :, pl.ds(pl.multiple_of(seq * width, width), width)],
            queries,
            load_sem.at[1],
        ),
        pltpu.make_async_copy(new_hbm, fresh, load_sem.at[2]),
    ]
    for load in loads:
        load.start()
    greet(shards, seq_count)
    for load in loads:
        load.wait()

    def rows_of(k):
        return k // 2, pl.ds((k % 2) * half, half)

    def z_copy(k, d):
        return pltpu.make_async_remote_copy(
            src_ref=outgoing.at[k, d - 1],
            dst_ref=landing[k].at[pl.ds((d - 1) * cap, cap)],
            send_sem=zsend.at[k, d - 1],
            recv_sem=zrecv.at[k, d - 1],
            device_id={"rep": rep ^ d},
            device_id_type=MESH,
        )

    far_first = sorted(range(1, rep_count), key=lambda d: -(d // 2 * 2))
    for k in range(PIECES):
        which, rows = rows_of(k)
        for d in far_first:

            def pack(j, carry, d=d, which=which, rows=rows, k=k):
                outgoing[k, d - 1, j] = kv[send_ref[d, j], which, rows, :]
                return carry

            lax.fori_loop(0, cap, pack, 0)
            z_copy(k, d).start()

        def keep(j, carry, which=which, rows=rows, k=k):
            landing[k][(rep_count - 1) * cap + j] = kv[send_ref[0, j], which, rows, :]
            return carry

        lax.fori_loop(0, landing[k].shape[0] - (rep_count - 1) * cap, keep, 0)

    length = length_ref[rep]
    slot_row = slot_ref[...]
    square = (requests, requests)
    first = lax.broadcasted_iota(jnp.int32, square, 0)
    second = lax.broadcasted_iota(jnp.int32, square, 1)
    slot_col = jnp.sum(
        jnp.where(first == second, slot_row.astype(jnp.float32), 0.0), axis=1, keepdims=True
    )
    hit_row = slot_row == rep
    hit_col = slot_col == rep.astype(jnp.float32)
    rank_row = jnp.sum(
        jnp.where(hit_col & (first < second), 1.0, 0.0), axis=0, keepdims=True
    ).astype(jnp.int32)
    score_scale = HD ** (-0.5)
    span = pages * page

    def tile(k, carry):
        want = k * ROWS + lax.broadcasted_iota(jnp.int32, (ROWS, requests), 0)
        pick = jnp.where((rank_row == want) & hit_row, 1.0, 0.0).astype(jnp.bfloat16)
        fresh_keys, fresh_values = [], []
        for t in range(steps):
            cosine, sine = cos_ref[t : t + 1, :], sin_ref[t : t + 1, :]
            picked = jnp.dot(pick, queries[t], preferred_element_type=jnp.float32)
            for g in range(group):
                head = turn(picked[:, g * HD : (g + 1) * HD], cosine, sine)
                at = (t * group + g) * ROWS
                rotated[at : at + ROWS, :] = head.astype(jnp.bfloat16)
            picked = jnp.dot(pick, fresh[0, t], preferred_element_type=jnp.float32)
            fresh_keys.append(turn(picked, cosine, sine).astype(jnp.bfloat16))
            picked = jnp.dot(pick, fresh[1, t], preferred_element_type=jnp.float32)
            fresh_values.append(picked.astype(jnp.bfloat16))
        fresh_keys = jnp.concatenate(fresh_keys, axis=0)
        fresh_values = jnp.concatenate(fresh_values, axis=0)
        scores = score_scale * lax.dot_general(
            rotated[...], fresh_keys, (((1,), (1,)), ((), ())), preferred_element_type=jnp.float32
        )
        row = lax.broadcasted_iota(jnp.int32, scores.shape, 0)
        column = lax.broadcasted_iota(jnp.int32, scores.shape, 1)
        allowed = (row % ROWS == column % ROWS) & (column // ROWS <= row // (group * ROWS))
        peak = jnp.max(jnp.where(allowed, scores, -1e30), axis=1, keepdims=True)
        weights = jnp.where(allowed, jnp.exp(scores - peak), 0.0)
        total = jnp.sum(weights, axis=1, keepdims=True)
        acc[...] = jnp.dot(
            weights.astype(jnp.bfloat16), fresh_values, preferred_element_type=jnp.float32
        )

        def chunk(c, state):
            peak, total = state
            part = pl.ds(pl.multiple_of(c * pages, pages), pages)
            scores = score_scale * lax.dot_general(
                rotated[...], kv[part, 0].reshape(span, HD), (((1,), (1,)), ((), ())),
                preferred_element_type=jnp.float32,
            )
            position = c * span + lax.broadcasted_iota(jnp.int32, (1, span), 1)
            scores = jnp.where(position < length, scores, -1e30)
            new_peak = jnp.maximum(peak, jnp.max(scores, axis=1, keepdims=True))
            weights = jnp.exp(scores - new_peak)
            factor = jnp.exp(peak - new_peak)
            total = total * factor + jnp.sum(weights, axis=1, keepdims=True)
            acc[...] = acc[...] * factor + jnp.dot(
                weights.astype(jnp.bfloat16), kv[part, 1].reshape(span, HD),
                preferred_element_type=jnp.float32,
            )
            return new_peak, total

        peak, total = lax.fori_loop(0, seq_count, chunk, (peak, total))
        result = (acc[...] / total).astype(jnp.bfloat16)
        here = pl.ds(pl.multiple_of(k * ROWS, ROWS), ROWS)
        for t in range(steps):
            for g in range(group):
                at = (t * group + g) * ROWS
                done[t, here, g * HD : (g + 1) * HD] = result[at : at + ROWS]
        return carry

    lax.fori_loop(0, tiles, tile, 0)

    plane = requests // rep_count
    packed = done.shape[1]
    order = lax.broadcasted_iota(jnp.int32, (1, requests), 1)
    spot = lax.broadcasted_iota(jnp.int32, (seats, packed), 0)
    source = lax.broadcasted_iota(jnp.int32, (seats, packed), 1)

    def o_copy(d):
        rows = pl.ds(d * seats, seats)
        return pltpu.make_async_remote_copy(
            src_ref=parts.at[:, rows],
            dst_ref=landed.at[:, rows],
            send_sem=osend.at[d],
            recv_sem=orecv.at[d],
            device_id={"rep": rep ^ d},
            device_id_type=MESH,
        )

    for d in far_first + [0]:
        begin = jnp.sum(
            jnp.where(hit_row & (order < (rep ^ d) * plane), 1.0, 0.0), axis=1, keepdims=True
        ).astype(jnp.int32)
        moved = jnp.where(source == spot + begin, 1.0, 0.0).astype(jnp.bfloat16)
        target = parts if d else landed
        for t in range(steps):
            target[t, d * seats : (d + 1) * seats] = jnp.dot(
                moved, done[t], preferred_element_type=jnp.float32
            ).astype(jnp.bfloat16)
        if d:
            o_copy(d).start()

    def p_copy(k, d):
        which, rows = rows_of(k)
        spot = pages_out.at[:, which, rows, pl.ds(pl.multiple_of(seq * HD, HD), HD)]
        if d == 0:
            return pltpu.make_async_copy(turned.at[k, 0], spot, psem.at[k])
        return pltpu.make_async_remote_copy(
            src_ref=turned.at[k, d],
            dst_ref=spot,
            send_sem=psend.at[k, d],
            recv_sem=precv.at[k, d],
            device_id={"seq": seq ^ d},
            device_id_type=MESH,
        )

    for k in range(PIECES):
        for d in far_first:
            z_copy(k, d).wait()
        for d in range(seq_count - 1, -1, -1):

            def sort(j, carry, d=d, k=k):
                turned[k, d, j] = landing[k][pick_ref[d, j]]
                return carry

            lax.fori_loop(0, pages, sort, 0)
            p_copy(k, d).start()

    owned = owned_out.shape[2]

    def a_copy(d):
        spot = attn_out.at[:, :, pl.ds(pl.multiple_of(seq * width, width), width)]
        if d == 0:
            return pltpu.make_async_copy(owned_out.at[seq], spot, asem)
        return pltpu.make_async_remote_copy(
            src_ref=owned_out.at[seq ^ d],
            dst_ref=spot,
            send_sem=asend.at[d],
            recv_sem=arecv.at[d],
            device_id={"seq": seq ^ d},
            device_id_type=MESH,
        )

    for d in far_first:
        o_copy(d).wait()
    chosen = lax.broadcasted_iota(jnp.int32, (plane, rep_count * seats), 1) == seat_ref[...]
    chosen = jnp.where(chosen, 1.0, 0.0).astype(jnp.bfloat16)
    for t in range(steps):
        spread = jnp.dot(chosen, landed[t], preferred_element_type=jnp.float32)
        for s in range(seq_count):
            owned_out[s, t] = spread[s * owned : (s + 1) * owned].astype(jnp.bfloat16)
    for d in range(seq_count - 1, -1, -1):
        a_copy(d).start()
    for k in range(PIECES):
        for d in range(seq_count):
            p_copy(k, d).wait()
    for d in range(seq_count):
        a_copy(d).wait()


def exchange(
    cap, seats, tiles, tables, lengths, slots, seat, cosine, sine, kv, queries, fresh, seq_count,
    rep_count, name, ident,
):
    send, pick = tables
    _, pages, _, page, _ = kv.shape
    blocks = seq_count * pages
    steps, requests, query_width = queries.shape
    width = query_width // seq_count
    rows = steps * (width // HD) * ROWS
    half = page // 2
    owned = requests // (rep_count * seq_count)
    anywhere = pl.BlockSpec(memory_space=pl.ANY)
    here = pl.BlockSpec(memory_space=pltpu.VMEM)
    numbers = pl.BlockSpec(memory_space=pltpu.SMEM)
    landing = (rep_count - 1) * cap + send.shape[1]
    sems = pltpu.SemaphoreType.DMA
    return pl.pallas_call(
        functools.partial(exchange_kernel, cap, seats, tiles, seq_count, rep_count),
        in_specs=[numbers] * 3 + [here] * 4 + [anywhere] * 3,
        out_specs=[anywhere, anywhere],
        out_shape=[
            jax.ShapeDtypeStruct((pages, 2, page, seq_count * HD), jnp.bfloat16),
            jax.ShapeDtypeStruct((steps, owned, query_width), jnp.bfloat16),
        ],
        scratch_shapes=[
            pltpu.VMEM((blocks, 2, page, HD), jnp.bfloat16),
            pltpu.VMEM((PIECES, rep_count - 1, cap, half, HD), jnp.bfloat16),
            pltpu.VMEM((PIECES, seq_count, pages, half, HD), jnp.bfloat16),
            pltpu.VMEM((steps, requests, width), jnp.bfloat16),
            pltpu.VMEM(fresh.shape, jnp.bfloat16),
            pltpu.VMEM((rows, HD), jnp.bfloat16),
            pltpu.VMEM((rows, HD), jnp.float32),
            pltpu.VMEM((steps, tiles * ROWS, width), jnp.bfloat16),
            pltpu.VMEM((steps, rep_count * seats, width), jnp.bfloat16),
            pltpu.VMEM((steps, rep_count * seats, width), jnp.bfloat16),
            pltpu.VMEM((seq_count, steps, owned, width), jnp.bfloat16),
            sems((3,)),
            sems((PIECES, rep_count)),
            sems((PIECES, rep_count)),
            sems((PIECES, seq_count)),
            sems((PIECES, seq_count)),
            sems((PIECES,)),
            sems((rep_count,)),
            sems((rep_count,)),
            sems((seq_count,)),
            sems((seq_count,)),
            sems(()),
        ]
        + [pltpu.VMEM((landing, half, HD), jnp.bfloat16)] * PIECES,
        compiler_params=pltpu.CompilerParams(
            vmem_limit_bytes=VMEM_BYTES, collective_id=ident, has_side_effects=True
        ),
        cost_estimate=pl.CostEstimate(
            flops=1, bytes_accessed=8 * 1024 * 1024, transcendentals=0
        ),
        name=name,
    )(
        send, pick, lengths, slots[None, :], seat, cosine, sine,
        kv.reshape(blocks, 2, page, HD), queries, fresh,
    )


def routes(page_table, cap, rep_index, seq_index, rep_count, seq_count):
    prompts, blocks = page_table.shape
    pages = blocks // seq_count
    most = blocks // 2
    plane = page_table // (pages * seq_count)
    block = jnp.arange(blocks, dtype=jnp.int32)
    same = (plane[:, :, None] == plane[:, None, :]) & (block[None, :, None] > block[None, None, :])
    rank = jnp.sum(same.astype(jnp.int32), axis=2)
    apart = jnp.arange(rep_count, dtype=jnp.int32)
    slot = jnp.arange(most, dtype=jnp.int32)
    own_plane = lax.dynamic_index_in_dim(plane, rep_index, 0, keepdims=False)
    own_rank = lax.dynamic_index_in_dim(rank, rep_index, 0, keepdims=False)
    match = (own_plane[None, None, :] == (rep_index ^ apart)[:, None, None]) & (
        own_rank[None, None, :] == slot[None, :, None]
    )
    send = jnp.sum(match.astype(jnp.int32) * block[None, None, :], axis=2)
    away = jnp.arange(prompts, dtype=jnp.int32) ^ rep_index
    origin = jnp.where(away == 0, (rep_count - 1), away - 1)
    spot = (origin[:, None] * cap + rank).reshape(-1)
    shard = rep_index * seq_count + (seq_index ^ jnp.arange(seq_count, dtype=jnp.int32))
    wanted = shard[:, None] * pages + jnp.arange(pages, dtype=jnp.int32)[None, :]
    found = (wanted[:, :, None] == page_table.reshape(-1)[None, None, :]).astype(jnp.int32)
    pick = jnp.sum(found * spot[None, None, :], axis=2)
    return send, pick


def seat_rows(request_slots, seats, rep_index, rep_count):
    plane = request_slots.shape[0] // rep_count
    mine = lax.dynamic_slice_in_dim(request_slots, rep_index * plane, plane, 0)
    index = jnp.arange(plane, dtype=jnp.int32)
    before = (mine[:, None] == mine[None, :]) & (index[None, :] < index[:, None])
    return (mine ^ rep_index)[:, None] * seats + jnp.sum(
        before.astype(jnp.int32), axis=1, keepdims=True
    )


def fits(page_table, request_slots, tiles, rep_count):
    prompts, blocks = page_table.shape
    each = jnp.arange(rep_count, dtype=jnp.int32)
    plane = page_table // blocks
    counts = jnp.sum((plane[:, None, :] == each[None, :, None]).astype(jnp.int32), axis=2)
    other = jnp.arange(prompts, dtype=jnp.int32)[:, None] != each[None, :]
    by_plane = request_slots.reshape(rep_count, -1)
    asked = jnp.sum((by_plane[None, :, :] == each[:, None, None]).astype(jnp.int32), axis=2)
    return (
        jnp.all((counts <= TIGHT) | ~other)
        & jnp.all(asked <= SEATS)
        & jnp.all(jnp.sum(asked, axis=1) <= tiles * ROWS)
    )


TIGHT = 12
SEATS = 16
TILES = 4


def attend_kernel(
    scalars, q_ref, new_ref, kv_ref, slot_row_ref, slot_col_ref, cos_ref, sin_ref, out_ref,
    rotated, acc, done,
):
    prompt, length = scalars[1], scalars[2]
    steps, requests, width = q_ref.shape
    group = width // HD
    paged = len(kv_ref.shape) == 5
    span = kv_ref.shape[1] * kv_ref.shape[3] if paged else kv_ref.shape[2]

    def source(c, which):
        if paged:
            return kv_ref[c, :, which].reshape(span, HD)
        return kv_ref[c, which]

    rows = steps * group * ROWS
    score_scale = HD ** (-0.5)

    hit_row = slot_row_ref[...] == prompt
    hit_col = slot_col_ref[...] == prompt
    square = (requests, requests)
    first = lax.broadcasted_iota(jnp.int32, square, 0)
    second = lax.broadcasted_iota(jnp.int32, square, 1)
    rank_row = jnp.sum(
        jnp.where(hit_col & (first < second), 1.0, 0.0), axis=0, keepdims=True
    ).astype(jnp.int32)
    rank_col = jnp.sum(
        jnp.where(hit_row & (second < first), 1.0, 0.0), axis=1, keepdims=True
    ).astype(jnp.int32)
    count = jnp.sum(jnp.where(hit_row, 1.0, 0.0)).astype(jnp.int32)
    done[...] = jnp.zeros_like(done)
    chunks = (length + span - 1) // span

    def tile(k, carry):
        want = k * ROWS + lax.broadcasted_iota(jnp.int32, (ROWS, requests), 0)
        pick = jnp.where((rank_row == want) & hit_row, 1.0, 0.0).astype(jnp.bfloat16)
        fresh_keys, fresh_values = [], []
        for t in range(steps):
            cosine, sine = cos_ref[t : t + 1, :], sin_ref[t : t + 1, :]
            picked = jnp.dot(pick, q_ref[t], preferred_element_type=jnp.float32)
            for g in range(group):
                head = turn(picked[:, g * HD : (g + 1) * HD], cosine, sine)
                at = (t * group + g) * ROWS
                rotated[at : at + ROWS, :] = head.astype(jnp.bfloat16)
            picked = jnp.dot(pick, new_ref[0, t], preferred_element_type=jnp.float32)
            fresh_keys.append(turn(picked, cosine, sine).astype(jnp.bfloat16))
            picked = jnp.dot(pick, new_ref[1, t], preferred_element_type=jnp.float32)
            fresh_values.append(picked.astype(jnp.bfloat16))
        fresh_keys = jnp.concatenate(fresh_keys, axis=0)
        fresh_values = jnp.concatenate(fresh_values, axis=0)
        scores = score_scale * lax.dot_general(
            rotated[...], fresh_keys, (((1,), (1,)), ((), ())), preferred_element_type=jnp.float32
        )
        row = lax.broadcasted_iota(jnp.int32, scores.shape, 0)
        column = lax.broadcasted_iota(jnp.int32, scores.shape, 1)
        allowed = (row % ROWS == column % ROWS) & (column // ROWS <= row // (group * ROWS))
        peak = jnp.max(jnp.where(allowed, scores, -1e30), axis=1, keepdims=True)
        weights = jnp.where(allowed, jnp.exp(scores - peak), 0.0)
        total = jnp.sum(weights, axis=1, keepdims=True)
        acc[...] = jnp.dot(
            weights.astype(jnp.bfloat16), fresh_values, preferred_element_type=jnp.float32
        )

        def chunk(c, state):
            peak, total = state
            scores = score_scale * lax.dot_general(
                rotated[...], source(c, 0), (((1,), (1,)), ((), ())),
                preferred_element_type=jnp.float32,
            )
            position = c * span + lax.broadcasted_iota(jnp.int32, (1, span), 1)
            scores = jnp.where(position < length, scores, -1e30)
            new_peak = jnp.maximum(peak, jnp.max(scores, axis=1, keepdims=True))
            weights = jnp.exp(scores - new_peak)
            factor = jnp.exp(peak - new_peak)
            total = total * factor + jnp.sum(weights, axis=1, keepdims=True)
            acc[...] = acc[...] * factor + jnp.dot(
                weights.astype(jnp.bfloat16), source(c, 1), preferred_element_type=jnp.float32
            )
            return new_peak, total

        peak, total = lax.fori_loop(0, chunks, chunk, (peak, total))
        result = (acc[...] / total).astype(jnp.bfloat16)
        here = pl.ds(pl.multiple_of(k * ROWS, ROWS), ROWS)
        for t in range(steps):
            for g in range(group):
                at = (t * group + g) * ROWS
                done[t, here, g * HD : (g + 1) * HD] = result[at : at + ROWS]
        return carry

    lax.fori_loop(0, (count + ROWS - 1) // ROWS, tile, 0)
    place = jnp.where((rank_col == second) & hit_col, 1.0, 0.0).astype(jnp.bfloat16)
    owned = out_ref.shape[2]
    for t in range(steps):
        spread = jnp.dot(place, done[t], preferred_element_type=jnp.float32)
        for d in range(out_ref.shape[0]):
            out_ref[d, t] = spread[d * owned : (d + 1) * owned].astype(jnp.bfloat16)


def attend(scalars, queries, new_kv, kv, slots, cosine, sine, shards, seq_count, fresh_split):
    steps, requests, query_width = queries.shape
    width = query_width // seq_count
    rows = steps * (width // HD) * ROWS
    padded = -(-requests // ROWS) * ROWS
    whole = lambda shape: pl.BlockSpec(shape, lambda i, s: (0,) * len(shape))
    fresh_index = (lambda i, s: (0, 0, 0, s[0])) if fresh_split else (lambda i, s: (0, 0, 0, 0))
    return pl.pallas_call(
        attend_kernel,
        grid_spec=pltpu.PrefetchScalarGridSpec(
            num_scalar_prefetch=1,
            grid=(1,),
            in_specs=[
                pl.BlockSpec((steps, requests, width), lambda i, s: (0, 0, s[0])),
                pl.BlockSpec((2, steps, requests, HD), fresh_index),
                whole(kv.shape),
                whole((1, requests)),
                whole((requests, 1)),
                whole(cosine.shape),
                whole(sine.shape),
            ],
            out_specs=whole((shards, steps, requests // shards, width)),
            scratch_shapes=[
                pltpu.VMEM((rows, HD), jnp.bfloat16),
                pltpu.VMEM((rows, HD), jnp.float32),
                pltpu.VMEM((steps, padded, width), jnp.bfloat16),
            ],
        ),
        out_shape=jax.ShapeDtypeStruct(
            (shards, steps, requests // shards, width), jnp.bfloat16
        ),
        compiler_params=pltpu.CompilerParams(vmem_limit_bytes=VMEM_BYTES),
        cost_estimate=pl.CostEstimate(
            flops=steps * requests * width * kv.size // (2 * HD),
            bytes_accessed=8 * 1024 * 1024,
            transcendentals=0,
        ),
        name="attend",
    )(scalars, queries, new_kv, kv, slots[None, :], slots[:, None], cosine, sine)


def fast_body(
    prompt_x, norm_gain, key_weight, value_weight, prompt_lengths, page_table, request_slots,
    queries, new_kv,
):
    seq_count = lax.axis_size("seq")
    rep_count = lax.axis_size("rep")
    rep_index = lax.axis_index("rep")
    seq_index = lax.axis_index("seq")
    shards = rep_count * seq_count
    blocks = page_table.shape[1]
    pages = blocks // seq_count
    page = prompt_x.shape[1] // pages
    steps, requests, _ = queries.shape
    own_length = prompt_lengths[0]
    for r in range(1, rep_count):
        own_length = jnp.where(rep_index == r, prompt_lengths[r], own_length)
    index = jnp.arange(page + pages + 8, dtype=jnp.int32)
    positions = jnp.where(
        index < page,
        index,
        jnp.where(
            index < page + pages,
            (seq_index * pages + index - page) * page,
            own_length + index - page - pages,
        ),
    )
    cosine, sine = angle_tables(positions.astype(jnp.float32))
    kv, all_new = stream(
        prompt_x[0], norm_gain[None, :], key_weight, value_weight, new_kv, cosine, sine, page,
        shards, seq_count,
    )
    most = blocks // 2
    plane = requests // rep_count
    sign = jnp.where(jnp.arange(HD, dtype=jnp.int32) % 2 == 0, -1.0, 1.0)
    first = page + pages
    step_cos, step_sin = cosine[first : first + steps], sine[first : first + steps] * sign

    def route(cap, seats, tiles, name, ident):
        tables = routes(page_table, cap, rep_index, seq_index, rep_count, seq_count)
        seat = seat_rows(request_slots, seats, rep_index, rep_count)

        def run(args):
            return exchange(
                cap, seats, tiles, tables, prompt_lengths, request_slots, seat, step_cos,
                step_sin, *args, seq_count, rep_count, name, ident,
            )

        return run

    paged_cache, attention = lax.cond(
        fits(page_table, request_slots, TILES, rep_count),
        route(TIGHT, SEATS, TILES, "exchange", 2),
        route(most, plane, -(-requests // ROWS), "exchange_full", 3),
        (kv, queries, all_new),
    )
    return (attention, paged_cache)


def quick(prompt_x, key_weight, page_table, new_kv):
    seq_count, rep_count = lax.axis_size("seq"), lax.axis_size("rep")
    heads = key_weight.shape[1] // HD
    powers = all(n & (n - 1) == 0 for n in (seq_count, rep_count))
    return (
        powers
        and key_weight.shape[1] % HD == 0
        and heads == seq_count
        and heads % 2 == 0
        and lax.axis_size("tp") * heads == KVH
        and prompt_x.shape[0] == 1
        and page_table.shape[0] == rep_count
        and prompt_x.shape[1] % BLOCK == 0
        and new_kv.shape[2] * seq_count * rep_count % (rep_count * ROWS) == 0
    )


def body(
    prompt_x,
    norm_gain,
    key_weight,
    value_weight,
    prompt_lengths,
    page_table,
    request_slots,
    queries,
    new_kv,
):
    seq_count = lax.axis_size("seq")
    rep_count = lax.axis_size("rep")
    tp_count = lax.axis_size("tp")
    rep_index = lax.axis_index("rep")
    seq_index = lax.axis_index("seq")
    tp_index = lax.axis_index("tp")
    shard_index = rep_index * seq_count + seq_index
    shard_count = rep_count * seq_count
    tokens = prompt_x.shape[1]
    if quick(prompt_x, key_weight, page_table, new_kv):
        return fast_body(
            prompt_x, norm_gain, key_weight, value_weight, prompt_lengths, page_table,
            request_slots, queries, new_kv,
        )
    prompts, blocks_per_prompt = page_table.shape
    pages_here = blocks_per_prompt // seq_count
    page = tokens // pages_here
    copies = max(1, tp_count // KVH)
    key_cols, value_cols = key_weight, value_weight
    if tp_count > KVH:
        other_key, other_value = swapped((key_weight, value_weight), "tp", 0)
        low_half = tp_index % 2 == 0
        key_cols = jnp.where(
            low_half,
            jnp.concatenate([key_weight, other_key], 1),
            jnp.concatenate([other_key, key_weight], 1),
        )
        value_cols = jnp.where(
            low_half,
            jnp.concatenate([value_weight, other_value], 1),
            jnp.concatenate([other_value, value_weight], 1),
        )
    head_width = key_cols.shape[1]
    heads_here = head_width // HD
    head_start = tp_index * heads_here // copies

    own_new = lax.dynamic_slice_in_dim(new_kv, head_start * HD, head_width, 3)
    all_new = lax.all_gather(own_new, ("rep", "seq"), axis=2, tiled=True)

    token_pos = (seq_index * tokens + jnp.arange(tokens, dtype=jnp.int32)).astype(jnp.float32)
    cosine, sine = rope_tables(token_pos)
    pages, heads = project(
        prompt_x[0], norm_gain[None, :], key_cols, value_cols, cosine, sine, page
    )

    by_head = heads_here == seq_count
    if by_head:
        kv = lax.all_to_all(heads, "seq", split_axis=0, concat_axis=0, tiled=True)
    else:
        kv = lax.all_gather(heads, "seq", axis=0, tiled=True)

    own_pages = lax.dynamic_slice(page_table, (rep_index, seq_index * pages_here), (1, pages_here))[0]
    hits = (
        own_pages[None, :] // pages_here == jnp.arange(shard_count, dtype=jnp.int32)[:, None]
    ).astype(jnp.int32)
    chosen = jnp.sum(hits * jnp.arange(pages_here, dtype=jnp.int32)[None, :], axis=1)
    outgoing = jnp.take(pages, chosen, axis=0, mode="clip")
    arrived = lax.all_to_all(outgoing, ("rep", "seq"), split_axis=0, concat_axis=0, tiled=True)
    page_ids = shard_index * pages_here + jnp.arange(pages_here, dtype=jnp.int32)
    flat_source = jnp.arange(prompts * blocks_per_prompt, dtype=jnp.int32) // pages_here
    matches = (page_table.reshape(-1)[None, :] == page_ids[:, None]).astype(jnp.int32)
    sources = jnp.sum(matches * flat_source[None, :], axis=1)
    paged_cache = jnp.take(arrived, sources, axis=0, mode="clip")

    own_length = lax.dynamic_index_in_dim(prompt_lengths, rep_index, 0, keepdims=False)
    steps = queries.shape[0]
    step_pos = (own_length + jnp.arange(steps, dtype=jnp.int32)).astype(jnp.float32)
    step_cos, step_sin = rope_tables(step_pos)
    scalars = jnp.stack([seq_index, rep_index, own_length]).astype(jnp.int32)
    partial = attend(
        scalars, queries, all_new, kv, request_slots, step_cos, step_sin, shard_count, seq_count,
        by_head,
    )
    owned = lax.all_to_all(partial, ("rep", "seq"), split_axis=0, concat_axis=0, tiled=True)
    attention = jnp.concatenate(
        [
            functools.reduce(
                jnp.add, [owned[r * seq_count + s] for r in range(rep_count)]
            )
            for s in range(seq_count)
        ],
        axis=-1,
    )
    return (attention, paged_cache)


def solution(mesh):
    in_specs = (
        P("rep", "seq", None),
        P(),
        P(None, "tp"),
        P(None, "tp"),
        P(),
        P(),
        P(),
        P(None, None, "tp"),
        P(None, None, ("rep", "seq"), None),
    )
    out_specs = (P(None, ("rep", "seq"), "tp"), P(("rep", "seq"), None, None, "tp"))
    return jax.shard_map(body, mesh=mesh, in_specs=in_specs, out_specs=out_specs, check_vma=False)
```

```python
import functools

import jax
import jax.numpy as jnp
import numpy as np
from jax import lax
from jax.experimental import pallas as pl
from jax.experimental.pallas import tpu as pltpu
from jax.sharding import PartitionSpec as P

KVH = 8
HD = 128
ROPE_BASE = 500000.0
EPS = 1e-05
VMEM_BYTES = 60 * 1024 * 1024


def swapped(value, axis, bit):
    mask = 2**bit
    pairs = [(source, source ^ mask) for source in range(lax.axis_size(axis))]
    return lax.ppermute(value, axis, pairs)


def rope_tables(positions):
    column = jnp.arange(HD, dtype=jnp.int32)
    within = (column - column % 2).astype(jnp.float32)
    inverse = jnp.exp(-(within / HD) * jnp.log(jnp.float32(ROPE_BASE)))
    angles = positions[:, None] * inverse[None, :]
    sign = jnp.where(column % 2 == 0, -1.0, 1.0)
    return jnp.cos(angles), jnp.sin(angles) * sign[None, :]


def turn(block, cosine, sine):
    lane = lax.broadcasted_iota(jnp.int32, block.shape, 1)
    neighbour = jnp.where(
        lane % 2 == 0, pltpu.roll(block, HD - 1, 1), pltpu.roll(block, 1, 1)
    )
    return block * cosine + neighbour * sine


def project_kernel(
    x_ref, gain_ref, wk_ref, wv_ref, cos_ref, sin_ref, pages_ref, heads_ref, key_acc, value_acc
):
    rows, width = x_ref.shape
    head_width = wk_ref.shape[1]
    depth = min(1024, width)
    steps = width // depth

    def squares(i, partial):
        chunk = x_ref[:, pl.ds(pl.multiple_of(i * depth, depth), depth)].astype(jnp.float32)
        chunk = chunk * chunk
        for j in range(depth // HD):
            partial = partial + chunk[:, j * HD : (j + 1) * HD]
        return partial

    partial = lax.fori_loop(0, steps, squares, jnp.zeros((rows, HD), jnp.float32))
    scale = lax.rsqrt(jnp.sum(partial, axis=1, keepdims=True) / width + EPS)
    key_acc[...] = jnp.zeros_like(key_acc)
    value_acc[...] = jnp.zeros_like(value_acc)

    def multiply(i, carry):
        part = pl.ds(pl.multiple_of(i * depth, depth), depth)
        normed = (x_ref[:, part].astype(jnp.float32) * scale * gain_ref[:, part]).astype(
            jnp.bfloat16
        )
        key_acc[...] += jnp.dot(normed, wk_ref[part, :], preferred_element_type=jnp.float32)
        value_acc[...] += jnp.dot(normed, wv_ref[part, :], preferred_element_type=jnp.float32)
        return carry

    lax.fori_loop(0, steps, multiply, 0)
    page = pages_ref.shape[2]
    for h in range(head_width // HD):
        cols = slice(h * HD, (h + 1) * HD)
        keys = turn(key_acc[:, cols], cos_ref[...], sin_ref[...]).astype(jnp.bfloat16)
        values = value_acc[:, cols].astype(jnp.bfloat16)
        heads_ref[h, 0] = keys
        heads_ref[h, 1] = values
        for b in range(rows // page):
            pages_ref[b, 0, :, cols] = keys[b * page : (b + 1) * page]
            pages_ref[b, 1, :, cols] = values[b * page : (b + 1) * page]


def project(x, gain, wk, wv, cosine, sine, page):
    tokens, width = x.shape
    head_width = wk.shape[1]
    heads = head_width // HD
    rows = min(256, tokens)
    return pl.pallas_call(
        project_kernel,
        grid=(tokens // rows,),
        in_specs=[
            pl.BlockSpec((rows, width), lambda i: (i, 0)),
            pl.BlockSpec((1, width), lambda i: (0, 0)),
            pl.BlockSpec((width, head_width), lambda i: (0, 0), pipeline_mode=pl.Buffered(1)),
            pl.BlockSpec((width, head_width), lambda i: (0, 0), pipeline_mode=pl.Buffered(1)),
            pl.BlockSpec((rows, HD), lambda i: (i, 0)),
            pl.BlockSpec((rows, HD), lambda i: (i, 0)),
        ],
        out_specs=[
            pl.BlockSpec((rows // page, 2, page, head_width), lambda i: (i, 0, 0, 0)),
            pl.BlockSpec((heads, 2, rows, HD), lambda i: (0, 0, i, 0)),
        ],
        out_shape=[
            jax.ShapeDtypeStruct((tokens // page, 2, page, head_width), jnp.bfloat16),
            jax.ShapeDtypeStruct((heads, 2, tokens, HD), jnp.bfloat16),
        ],
        scratch_shapes=[
            pltpu.VMEM((rows, head_width), jnp.float32),
            pltpu.VMEM((rows, head_width), jnp.float32),
        ],
        compiler_params=pltpu.CompilerParams(vmem_limit_bytes=VMEM_BYTES),
        cost_estimate=pl.CostEstimate(
            flops=4 * tokens * width * head_width,
            bytes_accessed=2 * tokens * width + 4 * width * head_width,
            transcendentals=0,
        ),
        name="project",
    )(x, gain, wk, wv, cosine, sine)


MESH = pl.DeviceIdType.MESH


def place_of(seq_count):
    return lax.axis_index("rep") * seq_count + lax.axis_index("seq")


def greet(shards, seq_count):
    me = place_of(seq_count)
    barrier = pltpu.get_barrier_semaphore()
    for i in range(1, shards):
        peer = lax.rem(me + i, shards)
        pl.semaphore_signal(
            barrier,
            inc=1,
            device_id={"rep": peer // seq_count, "seq": lax.rem(peer, seq_count)},
            device_id_type=MESH,
        )
    pl.semaphore_wait(barrier, shards - 1)


TIGHT = 12
SEATS = 16
TILES = 4
ROWS = 16


def power(n):
    return n.bit_length() - 1


def plan(table_ref, slot_ref, plan_out, rep_count, seq_count, rep, seq):
    prompts, blocks = table_ref.shape
    pages = blocks // seq_count
    most = blocks // 2
    requests = slot_ref.shape[1]
    table = table_ref[...].astype(jnp.float32)
    plane = jnp.floor(table * (1.0 / blocks))
    square = (blocks, blocks)
    above = lax.broadcasted_iota(jnp.int32, square, 0)
    across = lax.broadcasted_iota(jnp.int32, square, 1)
    index = lax.broadcasted_iota(jnp.int32, (blocks, 1), 0)
    shard = rep * seq_count + (seq ^ (index >> power(pages)))
    wanted = (shard * pages + (index & (pages - 1))).astype(jnp.float32)
    small = jnp.zeros((blocks, 1), jnp.float32)
    large = jnp.zeros((blocks, 1), jnp.float32)
    own_plane = jnp.zeros((1, blocks), jnp.float32)
    own_rank = jnp.zeros((1, blocks), jnp.float32)
    worst = jnp.zeros((1, 1), jnp.float32)
    for p in range(prompts):
        row = plane[p : p + 1, :]
        col = jnp.sum(jnp.where(above == across, row, 0.0), axis=1, keepdims=True)
        rank = jnp.sum(
            jnp.where((col == row) & (above < across), 1.0, 0.0), axis=0, keepdims=True
        )
        own_plane = own_plane + jnp.where(rep == p, row, 0.0)
        own_rank = own_rank + jnp.where(rep == p, rank, 0.0)
        away = rep ^ p
        origin = jnp.where(away == 0, rep_count - 1, away - 1).astype(jnp.float32)
        found = table[p : p + 1, :] == wanted
        small = small + jnp.sum(
            jnp.where(found, rank + origin * TIGHT, 0.0), axis=1, keepdims=True
        )
        large = large + jnp.sum(jnp.where(found, rank + origin * most, 0.0), axis=1, keepdims=True)
        for z in range(rep_count):
            if z != p:
                count = jnp.sum(jnp.where(row == z, 1.0, 0.0), axis=1, keepdims=True)
                worst = jnp.maximum(worst, count)
    slots = slot_ref[...]
    owner = lax.broadcasted_iota(jnp.int32, (1, requests), 1) >> power(requests // rep_count)
    asked = jnp.zeros((1, 1), jnp.float32)
    packed = jnp.zeros((1, 1), jnp.float32)
    for p in range(prompts):
        every = jnp.zeros((1, 1), jnp.float32)
        for z in range(rep_count):
            count = jnp.sum(
                jnp.where((slots == p) & (owner == z), 1.0, 0.0), axis=1, keepdims=True
            )
            asked = jnp.maximum(asked, count)
            every = every + count
        packed = jnp.maximum(packed, every)
    enough = (worst <= TIGHT) & (asked <= SEATS) & (packed <= TILES * ROWS)
    lanes = lax.broadcasted_iota(jnp.int32, (blocks, HD), 1)
    plan_out[:blocks] = jnp.where(
        lanes == 0, small, jnp.where(lanes == 1, large, 0.0)
    ).astype(jnp.int32)
    step = lax.broadcasted_iota(jnp.int32, (most, blocks), 0).astype(jnp.float32)
    number = lax.broadcasted_iota(jnp.int32, (most, blocks), 1).astype(jnp.float32)
    lanes = lax.broadcasted_iota(jnp.int32, (most, HD), 1)
    send = jnp.zeros((most, HD), jnp.float32)
    for d in range(rep_count):
        goal = (rep ^ d).astype(jnp.float32)
        match = (own_plane == goal) & (own_rank == step)
        column = jnp.sum(jnp.where(match, number, 0.0), axis=1, keepdims=True)
        send = send + jnp.where(lanes == d, column, 0.0)
    plan_out[blocks : blocks + most] = send.astype(jnp.int32)
    flag = jnp.where(enough, 1.0, 0.0) + jnp.zeros((8, HD), jnp.float32)
    plan_out[blocks + most :] = flag.astype(jnp.int32)


BLOCK = 256


def stream_kernel(
    shards, seq_count, page, length_ref, x_hbm, gain_ref, wk_hbm, wv_hbm, inverse_ref, table_ref,
    slot_ref, new_hbm, kv_out, new_out, plan_out, step_out, row_cos, row_sin, xs, wide, acc, chunk, xsem, wsem, ksend, krecv, own_sem, nsend, nrecv,
    nown,
):
    tokens, width = x_hbm.shape
    heads = wk_hbm.shape[1] // HD
    blocks = tokens // BLOCK
    pairs = heads // 2
    per_block = BLOCK // page
    me = place_of(seq_count)
    rep, seq = lax.axis_index("rep"), lax.axis_index("seq")
    order = [(heads // 2 + k) % heads for k in range(heads)]
    order = [o for o in order if o] + [0]
    head_of = [lax.rem(seq + o, heads) for o in order]

    def load_x(r):
        return pltpu.make_async_copy(x_hbm.at[pl.ds(r * BLOCK, BLOCK)], xs.at[pl.ds(r * BLOCK, BLOCK)], xsem.at[r])

    def load_w(k):
        cols = pl.ds(pl.multiple_of(head_of[k] * HD, HD), HD)
        at = (k % 2) * 2 * HD
        return [
            pltpu.make_async_copy(
                w.at[:, cols], wide.at[k // 2, :, pl.ds(at + j * HD, HD)], wsem.at[k, j]
            )
            for j, w in enumerate((wk_hbm, wv_hbm))
        ]

    load_x(0).start()
    for k in range(2):
        for copy in load_w(k):
            copy.start()
    for r in range(1, blocks):
        load_x(r).start()
    for k in range(2, heads):
        for copy in load_w(k):
            copy.start()

    greet(shards, seq_count)
    owned = new_hbm.shape[2]
    tp_head = lax.axis_index("tp") * heads

    def new_copy(i):
        peer = lax.rem(me + i, shards)
        peer_seq = lax.rem(peer, seq_count)
        cols = pl.ds(pl.multiple_of((tp_head + peer_seq) * HD, HD), HD)
        return pltpu.make_async_remote_copy(
            src_ref=new_hbm.at[:, :, :, cols],
            dst_ref=new_out.at[:, :, pl.ds(pl.multiple_of(me * owned, owned), owned), :],
            send_sem=nsend.at[i],
            recv_sem=nrecv.at[i],
            device_id={"rep": peer // seq_count, "seq": peer_seq},
            device_id_type=MESH,
        )

    for i in range(1, shards):
        new_copy(i).start()
    own_new = pltpu.make_async_copy(
        new_hbm.at[:, :, :, pl.ds(pl.multiple_of((tp_head + seq) * HD, HD), HD)],
        new_out.at[:, :, pl.ds(pl.multiple_of(me * owned, owned), owned), :],
        nown,
    )
    own_new.start()

    plan(table_ref, slot_ref, plan_out, shards // seq_count, seq_count, rep, seq)
    count = tokens // page
    inverse = inverse_ref[...]
    cells = lax.broadcasted_iota(jnp.int32, (page, HD), 0)
    bases = (seq * count + lax.broadcasted_iota(jnp.int32, (count, HD), 0)) * page
    later = length_ref[rep] + lax.broadcasted_iota(jnp.int32, (8, HD), 0)
    cell_angle = cells.astype(jnp.float32) * inverse
    base_angle = bases.astype(jnp.float32) * inverse
    step_angle = later.astype(jnp.float32) * inverse
    cell_cos, cell_sin = jnp.cos(cell_angle), jnp.sin(cell_angle)
    page_cos, page_sin = jnp.cos(base_angle), jnp.sin(base_angle)
    even_row = lax.broadcasted_iota(jnp.int32, (1, HD), 1) % 2 == 0
    step_sin = jnp.sin(step_angle)
    step_out[:8] = jnp.cos(step_angle)
    step_out[8:] = jnp.where(even_row, -step_sin, step_sin)
    for n in range(tokens // page):
        rows = slice(n * page, (n + 1) * page)
        base_cos, base_sin = page_cos[n : n + 1], page_sin[n : n + 1]
        row_cos[rows] = base_cos * cell_cos - base_sin * cell_sin
        sine = base_sin * cell_cos + base_cos * cell_sin
        row_sin[rows] = jnp.where(even_row, -sine, sine)

    sub = min(64, BLOCK)

    def norm(r):
        for q in range(r * BLOCK, (r + 1) * BLOCK, sub):
            row = slice(q, q + sub)
            partial = jnp.zeros((sub, HD), jnp.float32)
            for j in range(0, width, 4 * HD):
                piece = xs[row, j : j + 4 * HD].astype(jnp.float32)
                piece = piece * piece
                for s in range(4):
                    partial = partial + piece[:, s * HD : (s + 1) * HD]
            scale = lax.rsqrt(jnp.sum(partial, axis=1, keepdims=True) / width + EPS)
            for j in range(0, width, 4 * HD):
                cols = slice(j, j + 4 * HD)
                xs[row, cols] = (
                    xs[row, cols].astype(jnp.float32) * scale * gain_ref[:, cols]
                ).astype(jnp.bfloat16)

    def kv_copy(k, r):
        part = pl.ds(r * per_block, per_block)
        return pltpu.make_async_remote_copy(
            src_ref=chunk.at[k, part],
            dst_ref=kv_out.at[seq, part],
            send_sem=ksend.at[k, r],
            recv_sem=krecv.at[k, r],
            device_id={"seq": head_of[k]},
            device_id_type=MESH,
        )

    def own_copy(r):
        part = pl.ds(r * per_block, per_block)
        return pltpu.make_async_copy(
            chunk.at[heads - 1, part], kv_out.at[seq, part], own_sem.at[r]
        )

    lane = lax.broadcasted_iota(jnp.int32, (page, HD), 1)
    even = lane % 2 == 0

    def finish(k, r, at):
        for b in range(per_block):
            rows = slice(b * page, (b + 1) * page)
            n = r * per_block + b
            here = pl.ds(pl.multiple_of(n * page, page), page)
            keys = acc[rows, at : at + HD]
            neighbour = jnp.where(even, pltpu.roll(keys, HD - 1, 1), pltpu.roll(keys, 1, 1))
            chunk[k, n, 0] = (keys * row_cos[here] + neighbour * row_sin[here]).astype(
                jnp.bfloat16
            )
            chunk[k, n, 1] = acc[rows, at + HD : at + 2 * HD].astype(jnp.bfloat16)
        if k == heads - 1:
            own_copy(r).start()
        else:
            kv_copy(k, r).start()

    load_x(0).wait()
    norm(0)
    for k in range(2):
        for copy in load_w(k):
            copy.wait()
    for r in range(blocks):
        if r + 1 < blocks:
            load_x(r + 1).wait()
        if r:
            finish(0, r - 1, 0)
            finish(1, r - 1, 2 * HD)
        acc[...] = jnp.dot(
            xs[r * BLOCK : (r + 1) * BLOCK], wide[0], preferred_element_type=jnp.float32
        )
        if r + 1 < blocks:
            norm(r + 1)
    finish(0, blocks - 1, 0)
    finish(1, blocks - 1, 2 * HD)
    for pair in range(1, pairs):
        for k in (2 * pair, 2 * pair + 1):
            for copy in load_w(k):
                copy.wait()

        def rest(r, carry, pair=pair):
            rows = pl.ds(pl.multiple_of(r * BLOCK, BLOCK), BLOCK)
            acc[...] = jnp.dot(xs[rows], wide[pair], preferred_element_type=jnp.float32)
            finish(2 * pair, r, 0)
            finish(2 * pair + 1, r, 2 * HD)
            return carry

        lax.fori_loop(0, blocks, rest, 0)

    for r in range(blocks):
        own_copy(r).wait()
        for k in range(heads - 1):
            kv_copy(k, r).wait()
    own_new.wait()
    for i in range(1, shards):
        new_copy(i).wait()


def stream(
    x, gain, wk, wv, new_kv, lengths, page_table, slots, page, shards, seq_count
):
    tokens, width = x.shape
    heads = wk.shape[1] // HD
    blocks = tokens // BLOCK
    pages = tokens // page
    steps, owned = new_kv.shape[1:3]
    column = np.arange(HD)
    within = (column - column % 2) / HD
    inverse = jnp.asarray(np.exp(-within * np.log(ROPE_BASE))[None, :], jnp.float32)
    anywhere = pl.BlockSpec(memory_space=pl.ANY)
    here = pl.BlockSpec(memory_space=pltpu.VMEM)
    return pl.pallas_call(
        functools.partial(stream_kernel, shards, seq_count, page),
        in_specs=[pl.BlockSpec(memory_space=pltpu.SMEM)]
        + [anywhere, here, anywhere, anywhere, here, here, here, anywhere],
        out_specs=[anywhere, anywhere, here, here],
        out_shape=[
            jax.ShapeDtypeStruct((seq_count, pages, 2, page, HD), jnp.bfloat16),
            jax.ShapeDtypeStruct((2, steps, shards * owned, HD), jnp.bfloat16),
            jax.ShapeDtypeStruct((seq_count * pages * 3 // 2 + 8, HD), jnp.int32),
            jax.ShapeDtypeStruct((16, HD), jnp.float32),
        ],
        scratch_shapes=[
            pltpu.VMEM((tokens, HD), jnp.float32),
            pltpu.VMEM((tokens, HD), jnp.float32),
            pltpu.VMEM((tokens, width), jnp.bfloat16),
            pltpu.VMEM((heads // 2, width, 4 * HD), jnp.bfloat16),
            pltpu.VMEM((BLOCK, 4 * HD), jnp.float32),
            pltpu.VMEM((heads, pages, 2, page, HD), jnp.bfloat16),
            pltpu.SemaphoreType.DMA((blocks,)),
            pltpu.SemaphoreType.DMA((heads, 2)),
            pltpu.SemaphoreType.DMA((heads, blocks)),
            pltpu.SemaphoreType.DMA((heads, blocks)),
            pltpu.SemaphoreType.DMA((blocks,)),
            pltpu.SemaphoreType.DMA((shards,)),
            pltpu.SemaphoreType.DMA((shards,)),
            pltpu.SemaphoreType.DMA(()),
        ],
        compiler_params=pltpu.CompilerParams(
            vmem_limit_bytes=VMEM_BYTES, collective_id=1, has_side_effects=True
        ),
        cost_estimate=pl.CostEstimate(
            flops=4 * tokens * width * heads * HD,
            bytes_accessed=2 * tokens * width + 4 * width * heads * HD,
            transcendentals=0,
        ),
        name="stream",
    )(lengths, x, gain, wk, wv, inverse, page_table, slots[None, :], new_kv)


PIECES = 4


def exchange_kernel(
    cap, seats, tiles, lane, seq_count, rep_count, plan_ref, length_ref, slot_ref,
    turn_ref, kv_hbm, q_hbm, new_hbm, pages_out, attn_out,
    kv, outgoing, turned, queries, fresh, rotated, acc, done, parts, landed, owned_out,
    load_sem, zsend, zrecv, psend, precv, psem, osend, orecv, asend, arecv, asem, *landing,
):
    shards = seq_count * rep_count
    blocks, _, page, _ = kv.shape
    half = page // 2
    pages = blocks // seq_count
    steps, requests, width = queries.shape
    group = width // HD
    rep, seq = lax.axis_index("rep"), lax.axis_index("seq")
    loads = [
        pltpu.make_async_copy(kv_hbm, kv, load_sem.at[0]),
        pltpu.make_async_copy(
            q_hbm.at[:, :, pl.ds(pl.multiple_of(seq * width, width), width)],
            queries,
            load_sem.at[1],
        ),
        pltpu.make_async_copy(new_hbm, fresh, load_sem.at[2]),
    ]
    for load in loads:
        load.start()
    greet(shards, seq_count)
    for load in loads:
        load.wait()

    def rows_of(k):
        return k // 2, pl.ds((k % 2) * half, half)

    def z_copy(k, d):
        return pltpu.make_async_remote_copy(
            src_ref=outgoing.at[k, d - 1],
            dst_ref=landing[k].at[pl.ds((d - 1) * cap, cap)],
            send_sem=zsend.at[k, d - 1],
            recv_sem=zrecv.at[k, d - 1],
            device_id={"rep": rep ^ d},
            device_id_type=MESH,
        )

    far_first = sorted(range(1, rep_count), key=lambda d: -(d // 2 * 2))
    for k in range(PIECES):
        which, rows = rows_of(k)
        for d in far_first:

            def pack(j, carry, d=d, which=which, rows=rows, k=k):
                outgoing[k, d - 1, j] = kv[plan_ref[blocks + j, d], which, rows, :]
                return carry

            lax.fori_loop(0, cap, pack, 0)
            z_copy(k, d).start()

        def keep(j, carry, which=which, rows=rows, k=k):
            landing[k][(rep_count - 1) * cap + j] = kv[plan_ref[blocks + j, 0], which, rows, :]
            return carry

        lax.fori_loop(0, landing[k].shape[0] - (rep_count - 1) * cap, keep, 0)

    length = length_ref[rep]
    slot_row = slot_ref[...]
    square = (requests, requests)
    first = lax.broadcasted_iota(jnp.int32, square, 0)
    second = lax.broadcasted_iota(jnp.int32, square, 1)
    slot_col = jnp.sum(
        jnp.where(first == second, slot_row.astype(jnp.float32), 0.0), axis=1, keepdims=True
    )
    hit_row = slot_row == rep
    hit_col = slot_col == rep.astype(jnp.float32)
    rank_row = jnp.sum(
        jnp.where(hit_col & (first < second), 1.0, 0.0), axis=0, keepdims=True
    ).astype(jnp.int32)
    score_scale = HD ** (-0.5)
    span = pages * page

    def tile(k, carry):
        want = k * ROWS + lax.broadcasted_iota(jnp.int32, (ROWS, requests), 0)
        pick = jnp.where((rank_row == want) & hit_row, 1.0, 0.0).astype(jnp.bfloat16)
        fresh_keys, fresh_values = [], []
        for t in range(steps):
            cosine, sine = turn_ref[t : t + 1, :], turn_ref[8 + t : 9 + t, :]
            picked = jnp.dot(pick, queries[t], preferred_element_type=jnp.float32)
            for g in range(group):
                head = turn(picked[:, g * HD : (g + 1) * HD], cosine, sine)
                at = (t * group + g) * ROWS
                rotated[at : at + ROWS, :] = head.astype(jnp.bfloat16)
            picked = jnp.dot(pick, fresh[0, t], preferred_element_type=jnp.float32)
            fresh_keys.append(turn(picked, cosine, sine).astype(jnp.bfloat16))
            picked = jnp.dot(pick, fresh[1, t], preferred_element_type=jnp.float32)
            fresh_values.append(picked.astype(jnp.bfloat16))
        fresh_keys = jnp.concatenate(fresh_keys, axis=0)
        fresh_values = jnp.concatenate(fresh_values, axis=0)
        scores = score_scale * lax.dot_general(
            rotated[...], fresh_keys, (((1,), (1,)), ((), ())), preferred_element_type=jnp.float32
        )
        row = lax.broadcasted_iota(jnp.int32, scores.shape, 0)
        column = lax.broadcasted_iota(jnp.int32, scores.shape, 1)
        allowed = (row % ROWS == column % ROWS) & (column // ROWS <= row // (group * ROWS))
        peak = jnp.max(jnp.where(allowed, scores, -1e30), axis=1, keepdims=True)
        weights = jnp.where(allowed, jnp.exp(scores - peak), 0.0)
        total = jnp.sum(weights, axis=1, keepdims=True)
        acc[...] = jnp.dot(
            weights.astype(jnp.bfloat16), fresh_values, preferred_element_type=jnp.float32
        )

        def chunk(c, state):
            peak, total = state
            part = pl.ds(pl.multiple_of(c * pages, pages), pages)
            scores = score_scale * lax.dot_general(
                rotated[...], kv[part, 0].reshape(span, HD), (((1,), (1,)), ((), ())),
                preferred_element_type=jnp.float32,
            )
            position = c * span + lax.broadcasted_iota(jnp.int32, (1, span), 1)
            scores = jnp.where(position < length, scores, -1e30)
            new_peak = jnp.maximum(peak, jnp.max(scores, axis=1, keepdims=True))
            weights = jnp.exp(scores - new_peak)
            factor = jnp.exp(peak - new_peak)
            total = total * factor + jnp.sum(weights, axis=1, keepdims=True)
            acc[...] = acc[...] * factor + jnp.dot(
                weights.astype(jnp.bfloat16), kv[part, 1].reshape(span, HD),
                preferred_element_type=jnp.float32,
            )
            return new_peak, total

        peak, total = lax.fori_loop(0, seq_count, chunk, (peak, total))
        result = (acc[...] / total).astype(jnp.bfloat16)
        here = pl.ds(pl.multiple_of(k * ROWS, ROWS), ROWS)
        for t in range(steps):
            for g in range(group):
                at = (t * group + g) * ROWS
                done[t, here, g * HD : (g + 1) * HD] = result[at : at + ROWS]
        return carry

    lax.fori_loop(0, tiles, tile, 0)

    plane = requests // rep_count
    packed = done.shape[1]
    order = lax.broadcasted_iota(jnp.int32, (1, requests), 1)
    spot = lax.broadcasted_iota(jnp.int32, (seats, packed), 0)
    source = lax.broadcasted_iota(jnp.int32, (seats, packed), 1)

    def o_copy(d):
        rows = pl.ds(d * seats, seats)
        return pltpu.make_async_remote_copy(
            src_ref=parts.at[:, rows],
            dst_ref=landed.at[:, rows],
            send_sem=osend.at[d],
            recv_sem=orecv.at[d],
            device_id={"rep": rep ^ d},
            device_id_type=MESH,
        )

    for d in far_first + [0]:
        begin = jnp.sum(
            jnp.where(hit_row & (order < (rep ^ d) * plane), 1.0, 0.0), axis=1, keepdims=True
        ).astype(jnp.int32)
        moved = jnp.where(source == spot + begin, 1.0, 0.0).astype(jnp.bfloat16)
        target = parts if d else landed
        for t in range(steps):
            target[t, d * seats : (d + 1) * seats] = jnp.dot(
                moved, done[t], preferred_element_type=jnp.float32
            ).astype(jnp.bfloat16)
        if d:
            o_copy(d).start()

    def p_copy(k, d):
        which, rows = rows_of(k)
        spot = pages_out.at[:, which, rows, pl.ds(pl.multiple_of(seq * HD, HD), HD)]
        if d == 0:
            return pltpu.make_async_copy(turned.at[k, 0], spot, psem.at[k])
        return pltpu.make_async_remote_copy(
            src_ref=turned.at[k, d],
            dst_ref=spot,
            send_sem=psend.at[k, d],
            recv_sem=precv.at[k, d],
            device_id={"seq": seq ^ d},
            device_id_type=MESH,
        )

    for k in range(PIECES):
        for d in far_first:
            z_copy(k, d).wait()
        for d in range(seq_count - 1, -1, -1):

            def sort(j, carry, d=d, k=k):
                turned[k, d, j] = landing[k][plan_ref[d * pages + j, lane]]
                return carry

            lax.fori_loop(0, pages, sort, 0)
            p_copy(k, d).start()

    owned = owned_out.shape[2]

    def a_copy(d):
        spot = attn_out.at[:, :, pl.ds(pl.multiple_of(seq * width, width), width)]
        if d == 0:
            return pltpu.make_async_copy(owned_out.at[seq], spot, asem)
        return pltpu.make_async_remote_copy(
            src_ref=owned_out.at[seq ^ d],
            dst_ref=spot,
            send_sem=asend.at[d],
            recv_sem=arecv.at[d],
            device_id={"seq": seq ^ d},
            device_id_type=MESH,
        )

    for d in far_first:
        o_copy(d).wait()
    wide = (plane, requests)
    number = lax.broadcasted_iota(jnp.int32, wide, 1)
    mine = rep * plane + lax.broadcasted_iota(jnp.int32, wide, 0)
    prompt = jnp.sum(
        jnp.where(number == mine, slot_row.astype(jnp.float32), 0.0), axis=1, keepdims=True
    )
    ahead = (slot_row.astype(jnp.float32) == prompt) & (number >= rep * plane) & (number < mine)
    seat = jnp.sum(jnp.where(ahead, 1.0, 0.0), axis=1, keepdims=True).astype(jnp.int32)
    seat = seat + (prompt.astype(jnp.int32) ^ rep) * seats
    chosen = lax.broadcasted_iota(jnp.int32, (plane, rep_count * seats), 1) == seat
    chosen = jnp.where(chosen, 1.0, 0.0).astype(jnp.bfloat16)
    for t in range(steps):
        spread = jnp.dot(chosen, landed[t], preferred_element_type=jnp.float32)
        for s in range(seq_count):
            owned_out[s, t] = spread[s * owned : (s + 1) * owned].astype(jnp.bfloat16)
    for d in range(seq_count - 1, -1, -1):
        a_copy(d).start()
    for k in range(PIECES):
        for d in range(seq_count):
            p_copy(k, d).wait()
    for d in range(seq_count):
        a_copy(d).wait()


def exchange(
    cap, seats, tiles, lane, table, lengths, slots, turns, kv, queries, fresh, seq_count,
    rep_count, name, ident,
):
    _, pages, _, page, _ = kv.shape
    blocks = seq_count * pages
    steps, requests, query_width = queries.shape
    width = query_width // seq_count
    rows = steps * (width // HD) * ROWS
    half = page // 2
    owned = requests // (rep_count * seq_count)
    anywhere = pl.BlockSpec(memory_space=pl.ANY)
    here = pl.BlockSpec(memory_space=pltpu.VMEM)
    numbers = pl.BlockSpec(memory_space=pltpu.SMEM)
    landing = (rep_count - 1) * cap + blocks // 2
    sems = pltpu.SemaphoreType.DMA
    return pl.pallas_call(
        functools.partial(exchange_kernel, cap, seats, tiles, lane, seq_count, rep_count),
        in_specs=[numbers] * 2 + [here] * 2 + [anywhere] * 3,
        out_specs=[anywhere, anywhere],
        out_shape=[
            jax.ShapeDtypeStruct((pages, 2, page, seq_count * HD), jnp.bfloat16),
            jax.ShapeDtypeStruct((steps, owned, query_width), jnp.bfloat16),
        ],
        scratch_shapes=[
            pltpu.VMEM((blocks, 2, page, HD), jnp.bfloat16),
            pltpu.VMEM((PIECES, rep_count - 1, cap, half, HD), jnp.bfloat16),
            pltpu.VMEM((PIECES, seq_count, pages, half, HD), jnp.bfloat16),
            pltpu.VMEM((steps, requests, width), jnp.bfloat16),
            pltpu.VMEM(fresh.shape, jnp.bfloat16),
            pltpu.VMEM((rows, HD), jnp.bfloat16),
            pltpu.VMEM((rows, HD), jnp.float32),
            pltpu.VMEM((steps, tiles * ROWS, width), jnp.bfloat16),
            pltpu.VMEM((steps, rep_count * seats, width), jnp.bfloat16),
            pltpu.VMEM((steps, rep_count * seats, width), jnp.bfloat16),
            pltpu.VMEM((seq_count, steps, owned, width), jnp.bfloat16),
            sems((3,)),
            sems((PIECES, rep_count)),
            sems((PIECES, rep_count)),
            sems((PIECES, seq_count)),
            sems((PIECES, seq_count)),
            sems((PIECES,)),
            sems((rep_count,)),
            sems((rep_count,)),
            sems((seq_count,)),
            sems((seq_count,)),
            sems(()),
        ]
        + [pltpu.VMEM((landing, half, HD), jnp.bfloat16)] * PIECES,
        compiler_params=pltpu.CompilerParams(
            vmem_limit_bytes=VMEM_BYTES, collective_id=ident, has_side_effects=True
        ),
        cost_estimate=pl.CostEstimate(
            flops=1, bytes_accessed=8 * 1024 * 1024, transcendentals=0
        ),
        name=name,
    )(
        table, lengths, slots[None, :], turns,
        kv.reshape(blocks, 2, page, HD), queries, fresh,
    )


def attend_kernel(
    scalars, q_ref, new_ref, kv_ref, slot_row_ref, slot_col_ref, cos_ref, sin_ref, out_ref,
    rotated, acc, done,
):
    prompt, length = scalars[1], scalars[2]
    steps, requests, width = q_ref.shape
    group = width // HD
    paged = len(kv_ref.shape) == 5
    span = kv_ref.shape[1] * kv_ref.shape[3] if paged else kv_ref.shape[2]

    def source(c, which):
        if paged:
            return kv_ref[c, :, which].reshape(span, HD)
        return kv_ref[c, which]

    rows = steps * group * ROWS
    score_scale = HD ** (-0.5)

    hit_row = slot_row_ref[...] == prompt
    hit_col = slot_col_ref[...] == prompt
    square = (requests, requests)
    first = lax.broadcasted_iota(jnp.int32, square, 0)
    second = lax.broadcasted_iota(jnp.int32, square, 1)
    rank_row = jnp.sum(
        jnp.where(hit_col & (first < second), 1.0, 0.0), axis=0, keepdims=True
    ).astype(jnp.int32)
    rank_col = jnp.sum(
        jnp.where(hit_row & (second < first), 1.0, 0.0), axis=1, keepdims=True
    ).astype(jnp.int32)
    count = jnp.sum(jnp.where(hit_row, 1.0, 0.0)).astype(jnp.int32)
    done[...] = jnp.zeros_like(done)
    chunks = (length + span - 1) // span

    def tile(k, carry):
        want = k * ROWS + lax.broadcasted_iota(jnp.int32, (ROWS, requests), 0)
        pick = jnp.where((rank_row == want) & hit_row, 1.0, 0.0).astype(jnp.bfloat16)
        fresh_keys, fresh_values = [], []
        for t in range(steps):
            cosine, sine = cos_ref[t : t + 1, :], sin_ref[t : t + 1, :]
            picked = jnp.dot(pick, q_ref[t], preferred_element_type=jnp.float32)
            for g in range(group):
                head = turn(picked[:, g * HD : (g + 1) * HD], cosine, sine)
                at = (t * group + g) * ROWS
                rotated[at : at + ROWS, :] = head.astype(jnp.bfloat16)
            picked = jnp.dot(pick, new_ref[0, t], preferred_element_type=jnp.float32)
            fresh_keys.append(turn(picked, cosine, sine).astype(jnp.bfloat16))
            picked = jnp.dot(pick, new_ref[1, t], preferred_element_type=jnp.float32)
            fresh_values.append(picked.astype(jnp.bfloat16))
        fresh_keys = jnp.concatenate(fresh_keys, axis=0)
        fresh_values = jnp.concatenate(fresh_values, axis=0)
        scores = score_scale * lax.dot_general(
            rotated[...], fresh_keys, (((1,), (1,)), ((), ())), preferred_element_type=jnp.float32
        )
        row = lax.broadcasted_iota(jnp.int32, scores.shape, 0)
        column = lax.broadcasted_iota(jnp.int32, scores.shape, 1)
        allowed = (row % ROWS == column % ROWS) & (column // ROWS <= row // (group * ROWS))
        peak = jnp.max(jnp.where(allowed, scores, -1e30), axis=1, keepdims=True)
        weights = jnp.where(allowed, jnp.exp(scores - peak), 0.0)
        total = jnp.sum(weights, axis=1, keepdims=True)
        acc[...] = jnp.dot(
            weights.astype(jnp.bfloat16), fresh_values, preferred_element_type=jnp.float32
        )

        def chunk(c, state):
            peak, total = state
            scores = score_scale * lax.dot_general(
                rotated[...], source(c, 0), (((1,), (1,)), ((), ())),
                preferred_element_type=jnp.float32,
            )
            position = c * span + lax.broadcasted_iota(jnp.int32, (1, span), 1)
            scores = jnp.where(position < length, scores, -1e30)
            new_peak = jnp.maximum(peak, jnp.max(scores, axis=1, keepdims=True))
            weights = jnp.exp(scores - new_peak)
            factor = jnp.exp(peak - new_peak)
            total = total * factor + jnp.sum(weights, axis=1, keepdims=True)
            acc[...] = acc[...] * factor + jnp.dot(
                weights.astype(jnp.bfloat16), source(c, 1), preferred_element_type=jnp.float32
            )
            return new_peak, total

        peak, total = lax.fori_loop(0, chunks, chunk, (peak, total))
        result = (acc[...] / total).astype(jnp.bfloat16)
        here = pl.ds(pl.multiple_of(k * ROWS, ROWS), ROWS)
        for t in range(steps):
            for g in range(group):
                at = (t * group + g) * ROWS
                done[t, here, g * HD : (g + 1) * HD] = result[at : at + ROWS]
        return carry

    lax.fori_loop(0, (count + ROWS - 1) // ROWS, tile, 0)
    place = jnp.where((rank_col == second) & hit_col, 1.0, 0.0).astype(jnp.bfloat16)
    owned = out_ref.shape[2]
    for t in range(steps):
        spread = jnp.dot(place, done[t], preferred_element_type=jnp.float32)
        for d in range(out_ref.shape[0]):
            out_ref[d, t] = spread[d * owned : (d + 1) * owned].astype(jnp.bfloat16)


def attend(scalars, queries, new_kv, kv, slots, cosine, sine, shards, seq_count, fresh_split):
    steps, requests, query_width = queries.shape
    width = query_width // seq_count
    rows = steps * (width // HD) * ROWS
    padded = -(-requests // ROWS) * ROWS
    whole = lambda shape: pl.BlockSpec(shape, lambda i, s: (0,) * len(shape))
    fresh_index = (lambda i, s: (0, 0, 0, s[0])) if fresh_split else (lambda i, s: (0, 0, 0, 0))
    return pl.pallas_call(
        attend_kernel,
        grid_spec=pltpu.PrefetchScalarGridSpec(
            num_scalar_prefetch=1,
            grid=(1,),
            in_specs=[
                pl.BlockSpec((steps, requests, width), lambda i, s: (0, 0, s[0])),
                pl.BlockSpec((2, steps, requests, HD), fresh_index),
                whole(kv.shape),
                whole((1, requests)),
                whole((requests, 1)),
                whole(cosine.shape),
                whole(sine.shape),
            ],
            out_specs=whole((shards, steps, requests // shards, width)),
            scratch_shapes=[
                pltpu.VMEM((rows, HD), jnp.bfloat16),
                pltpu.VMEM((rows, HD), jnp.float32),
                pltpu.VMEM((steps, padded, width), jnp.bfloat16),
            ],
        ),
        out_shape=jax.ShapeDtypeStruct(
            (shards, steps, requests // shards, width), jnp.bfloat16
        ),
        compiler_params=pltpu.CompilerParams(vmem_limit_bytes=VMEM_BYTES),
        cost_estimate=pl.CostEstimate(
            flops=steps * requests * width * kv.size // (2 * HD),
            bytes_accessed=8 * 1024 * 1024,
            transcendentals=0,
        ),
        name="attend",
    )(scalars, queries, new_kv, kv, slots[None, :], slots[:, None], cosine, sine)


def fast_body(
    prompt_x, norm_gain, key_weight, value_weight, prompt_lengths, page_table, request_slots,
    queries, new_kv,
):
    seq_count = lax.axis_size("seq")
    rep_count = lax.axis_size("rep")
    shards = rep_count * seq_count
    blocks = page_table.shape[1]
    pages = blocks // seq_count
    page = prompt_x.shape[1] // pages
    steps, requests, _ = queries.shape
    kv, all_new, table, turns = stream(
        prompt_x[0], norm_gain[None, :], key_weight, value_weight, new_kv, prompt_lengths,
        page_table, request_slots, page, shards, seq_count,
    )
    most = blocks // 2
    plane = requests // rep_count
    def route(cap, seats, tiles, lane, name, ident):
        def run(args):
            return exchange(
                cap, seats, tiles, lane, table, prompt_lengths, request_slots, turns, *args, seq_count,
                rep_count, name, ident,
            )

        return run

    paged_cache, attention = lax.cond(
        table[blocks + most, 0] > 0,
        route(TIGHT, SEATS, TILES, 0, "exchange", 2),
        route(most, plane, -(-requests // ROWS), 1, "exchange_full", 3),
        (kv, queries, all_new),
    )
    return (attention, paged_cache)


def quick(prompt_x, key_weight, page_table, new_kv):
    seq_count, rep_count = lax.axis_size("seq"), lax.axis_size("rep")
    heads = key_weight.shape[1] // HD
    powers = all(
        n & (n - 1) == 0 for n in (seq_count, rep_count, new_kv.shape[2] * seq_count)
    )
    return (
        powers
        and page_table.shape[1] & (page_table.shape[1] - 1) == 0
        and page_table.shape[1] % (2 * seq_count) == 0
        and key_weight.shape[1] % HD == 0
        and heads == seq_count
        and heads % 2 == 0
        and lax.axis_size("tp") * heads == KVH
        and prompt_x.shape[0] == 1
        and page_table.shape[0] == rep_count
        and prompt_x.shape[1] % BLOCK == 0
        and new_kv.shape[1] <= 8
        and new_kv.shape[2] * seq_count * rep_count % (rep_count * ROWS) == 0
    )


def body(
    prompt_x,
    norm_gain,
    key_weight,
    value_weight,
    prompt_lengths,
    page_table,
    request_slots,
    queries,
    new_kv,
):
    seq_count = lax.axis_size("seq")
    rep_count = lax.axis_size("rep")
    tp_count = lax.axis_size("tp")
    rep_index = lax.axis_index("rep")
    seq_index = lax.axis_index("seq")
    tp_index = lax.axis_index("tp")
    shard_index = rep_index * seq_count + seq_index
    shard_count = rep_count * seq_count
    tokens = prompt_x.shape[1]
    if quick(prompt_x, key_weight, page_table, new_kv):
        return fast_body(
            prompt_x, norm_gain, key_weight, value_weight, prompt_lengths, page_table,
            request_slots, queries, new_kv,
        )
    prompts, blocks_per_prompt = page_table.shape
    pages_here = blocks_per_prompt // seq_count
    page = tokens // pages_here
    copies = max(1, tp_count // KVH)
    key_cols, value_cols = key_weight, value_weight
    if tp_count > KVH:
        other_key, other_value = swapped((key_weight, value_weight), "tp", 0)
        low_half = tp_index % 2 == 0
        key_cols = jnp.where(
            low_half,
            jnp.concatenate([key_weight, other_key], 1),
            jnp.concatenate([other_key, key_weight], 1),
        )
        value_cols = jnp.where(
            low_half,
            jnp.concatenate([value_weight, other_value], 1),
            jnp.concatenate([other_value, value_weight], 1),
        )
    head_width = key_cols.shape[1]
    heads_here = head_width // HD
    head_start = tp_index * heads_here // copies

    own_new = lax.dynamic_slice_in_dim(new_kv, head_start * HD, head_width, 3)
    all_new = lax.all_gather(own_new, ("rep", "seq"), axis=2, tiled=True)

    token_pos = (seq_index * tokens + jnp.arange(tokens, dtype=jnp.int32)).astype(jnp.float32)
    cosine, sine = rope_tables(token_pos)
    pages, heads = project(
        prompt_x[0], norm_gain[None, :], key_cols, value_cols, cosine, sine, page
    )

    by_head = heads_here == seq_count
    if by_head:
        kv = lax.all_to_all(heads, "seq", split_axis=0, concat_axis=0, tiled=True)
    else:
        kv = lax.all_gather(heads, "seq", axis=0, tiled=True)

    own_pages = lax.dynamic_slice(page_table, (rep_index, seq_index * pages_here), (1, pages_here))[0]
    hits = (
        own_pages[None, :] // pages_here == jnp.arange(shard_count, dtype=jnp.int32)[:, None]
    ).astype(jnp.int32)
    chosen = jnp.sum(hits * jnp.arange(pages_here, dtype=jnp.int32)[None, :], axis=1)
    outgoing = jnp.take(pages, chosen, axis=0, mode="clip")
    arrived = lax.all_to_all(outgoing, ("rep", "seq"), split_axis=0, concat_axis=0, tiled=True)
    page_ids = shard_index * pages_here + jnp.arange(pages_here, dtype=jnp.int32)
    flat_source = jnp.arange(prompts * blocks_per_prompt, dtype=jnp.int32) // pages_here
    matches = (page_table.reshape(-1)[None, :] == page_ids[:, None]).astype(jnp.int32)
    sources = jnp.sum(matches * flat_source[None, :], axis=1)
    paged_cache = jnp.take(arrived, sources, axis=0, mode="clip")

    own_length = lax.dynamic_index_in_dim(prompt_lengths, rep_index, 0, keepdims=False)
    steps = queries.shape[0]
    step_pos = (own_length + jnp.arange(steps, dtype=jnp.int32)).astype(jnp.float32)
    step_cos, step_sin = rope_tables(step_pos)
    scalars = jnp.stack([seq_index, rep_index, own_length]).astype(jnp.int32)
    partial = attend(
        scalars, queries, all_new, kv, request_slots, step_cos, step_sin, shard_count, seq_count,
        by_head,
    )
    owned = lax.all_to_all(partial, ("rep", "seq"), split_axis=0, concat_axis=0, tiled=True)
    attention = jnp.concatenate(
        [
            functools.reduce(
                jnp.add, [owned[r * seq_count + s] for r in range(rep_count)]
            )
            for s in range(seq_count)
        ],
        axis=-1,
    )
    return (attention, paged_cache)


def solution(mesh):
    in_specs = (
        P("rep", "seq", None),
        P(),
        P(None, "tp"),
        P(None, "tp"),
        P(),
        P(),
        P(),
        P(None, None, "tp"),
        P(None, None, ("rep", "seq"), None),
    )
    out_specs = (P(None, ("rep", "seq"), "tp"), P(("rep", "seq"), None, None, "tp"))
    return jax.shard_map(body, mesh=mesh, in_specs=in_specs, out_specs=out_specs, check_vma=False)
```
